128 devices in a mesh: tables: 1, g: 128 (over z, y, x, core).
Axes of the slice: x: 4, y: 4, z: 4, core: 2. Of those that a mesh axis runs over, the one named last changes fastest.
Arguments:
- item_factors: float32 [262144, 64], P(('tables', 'g'))
- user_start: float32 [65536, 64], P(('tables', 'g'))
- by_item_idx: int32 [128, 65536, 8], P(('tables', 'g'))
- by_item_conf: float32 [128, 65536, 8], P(('tables', 'g'))
- by_user_idx: int32 [128, 262144, 2], P(('tables', 'g'))
- by_user_conf: float32 [128, 262144, 2], P(('tables', 'g'))
Outputs:
- output 1: float32 [65536, 64], P(('tables', 'g'))
- output 2: float32 [262144, 64], P(('tables', 'g'))
All inputs are finite; a program needn't handle non-finite values.
Results may differ from the reference program's by a relative error of at most 0.0123.
Values are sent between devices in bfloat16 or wider.
A program may use at most 1 GiB of HBM per device.

```python
import jax
import jax.numpy as jnp
from jax import lax

GROUP_SIZE = 128
USERS_DEV = 512
ITEMS_DEV = 2048
USER_SLOTS = 8
FACTORS = 64
CG_STEPS = 3

ITEM_SLOTS = max(1, USERS_DEV * USER_SLOTS // ITEMS_DEV)
NUM_USERS = GROUP_SIZE * USERS_DEV
NUM_ITEMS = GROUP_SIZE * ITEMS_DEV
REG_LAMBDA = 0.01
FULL_PREC = lax.Precision.HIGHEST


def draw_layout(layout_key):
    key_lvl, key_cnt, key_home, key_mult, key_shift = jax.random.split(layout_key, 5)
    shard_lvl = jax.random.randint(key_lvl, (GROUP_SIZE, 1), 1, 5)
    count_draws = jax.random.randint(key_cnt, (3, GROUP_SIZE, NUM_USERS), 0, USER_SLOTS + 1)
    counts = jnp.minimum(USER_SLOTS, count_draws[0] * count_draws[1] * count_draws[2] * shard_lvl // (2 * USER_SLOTS * USER_SLOTS))
    home_shard = jax.random.randint(key_home, (1, NUM_USERS), 0, GROUP_SIZE)
    counts = jnp.where(jnp.arange(GROUP_SIZE)[:, None] == home_shard, USER_SLOTS, counts)
    stride_mul = 2 * jax.random.randint(key_mult, (GROUP_SIZE, GROUP_SIZE, 1, 1), 0, ITEMS_DEV // 2) + 1
    offset_add = jax.random.randint(key_shift, (GROUP_SIZE, GROUP_SIZE, 1, 1), 0, ITEMS_DEV)
    flat_slot = jnp.arange(USERS_DEV)[:, None] * USER_SLOTS + jnp.arange(USER_SLOTS)[None, :]
    item_local = (stride_mul * (flat_slot % ITEMS_DEV) + offset_add) % ITEMS_DEV
    observed = jnp.arange(USER_SLOTS) < counts.reshape(GROUP_SIZE, GROUP_SIZE, USERS_DEV, 1)
    rep_slot = flat_slot // ITEMS_DEV
    return item_local, observed, rep_slot


def setup_inputs(seed: int = 0, part: int = 0) -> dict:
    base_key = jax.random.fold_in(jax.random.key(seed), part)
    key_lay, key_rate, key_item, key_user, key_fill = jax.random.split(base_key, 5)
    item_local, observed, rep_slot = draw_layout(key_lay)
    ratings = jax.random.randint(key_rate, item_local.shape, 1, 6)
    conf_vals = jnp.where(observed, 1.0 + 10.0 * ratings.astype(jnp.float32), 0.0)
    col_scale = 2.0 ** (-4.0 * jnp.arange(FACTORS, dtype=jnp.float32) / FACTORS)
    item_factors = jax.random.normal(key_item, (NUM_ITEMS, FACTORS), jnp.float32) * col_scale / (NUM_ITEMS ** 0.5)
    user_start = jax.random.normal(key_user, (NUM_USERS, FACTORS), jnp.float32)
    dst_shard = jnp.arange(GROUP_SIZE).reshape(1, GROUP_SIZE, 1, 1)
    item_pos = jnp.arange(GROUP_SIZE).reshape(GROUP_SIZE, 1, 1, 1) * ITEMS_DEV + item_local
    user_local = jnp.broadcast_to(jnp.arange(USERS_DEV).reshape(1, 1, USERS_DEV, 1), item_local.shape)
    by_user_idx = jax.random.randint(key_fill, (GROUP_SIZE, NUM_ITEMS, ITEM_SLOTS), 0, USERS_DEV)
    by_user_idx = by_user_idx.at[dst_shard, item_pos, rep_slot].set(user_local)
    by_user_conf = jnp.zeros((GROUP_SIZE, NUM_ITEMS, ITEM_SLOTS), jnp.float32).at[dst_shard, item_pos, rep_slot].set(conf_vals)
    return {'item_factors': item_factors, 'user_start': user_start,
            'by_item_idx': item_local.reshape(GROUP_SIZE, NUM_USERS, USER_SLOTS),
            'by_item_conf': conf_vals.reshape(GROUP_SIZE, NUM_USERS, USER_SLOTS),
            'by_user_idx': by_user_idx, 'by_user_conf': by_user_conf}


def cg_solve(gram_reg, normal_mats, rhs_vec, warm_start):
    def apply_mat(vectors):
        return jnp.dot(vectors, gram_reg, precision=FULL_PREC) + jnp.einsum('nab,nb->na', normal_mats, vectors, precision=FULL_PREC)

    residual = rhs_vec - apply_mat(warm_start)
    res_sq = jnp.sum(residual * residual, axis=-1, keepdims=True)

    def cg_step(cg_state, unused):
        approx, residual, search_dir, res_sq = cg_state
        mat_dir = apply_mat(search_dir)
        step_len = res_sq / jnp.sum(search_dir * mat_dir, axis=-1, keepdims=True)
        approx = approx + step_len * search_dir
        residual = residual - step_len * mat_dir
        new_sq = jnp.sum(residual * residual, axis=-1, keepdims=True)
        search_dir = residual + (new_sq / res_sq) * search_dir
        return (approx, residual, search_dir, new_sq), None

    final_state, unused = lax.scan(cg_step, (warm_start, residual, residual, res_sq), None, length=CG_STEPS)
    return final_state[0]


def solve_rows(gathered, conf_blk, gram_reg, warm_start):
    weights = jnp.maximum(conf_blk - 1.0, 0.0)[..., None]
    w_rows = (weights * gathered).astype(jnp.bfloat16).astype(jnp.float32)
    obs_mask = (conf_blk > 0.0).astype(jnp.float32)[..., None]
    normal_mats = jnp.einsum('dnsa,dnsb->nab', w_rows, gathered, precision=FULL_PREC)
    rhs_vec = jnp.sum(w_rows + obs_mask * gathered, axis=(0, 2))
    return cg_solve(gram_reg, normal_mats, rhs_vec, warm_start)


def reference(item_factors, user_start, by_item_idx, by_item_conf, by_user_idx, by_user_conf):
    reg_eye = REG_LAMBDA * jnp.eye(FACTORS, dtype=jnp.float32)
    item_bf = item_factors.astype(jnp.bfloat16).astype(jnp.float32)
    gram_items = jnp.dot(item_bf.T, item_bf, precision=FULL_PREC) + reg_eye
    item_base = (jnp.arange(GROUP_SIZE) * ITEMS_DEV).reshape(GROUP_SIZE, 1, 1, 1)
    item_idx = (by_item_idx.reshape(GROUP_SIZE, GROUP_SIZE, USERS_DEV, USER_SLOTS) + item_base).transpose(1, 0, 2, 3)
    item_conf = by_item_conf.reshape(GROUP_SIZE, GROUP_SIZE, USERS_DEV, USER_SLOTS).transpose(1, 0, 2, 3)

    def solve_owner(owner_args):
        global_idx, conf_blk, warm_start = owner_args
        return solve_rows(item_bf[global_idx], conf_blk, gram_items, warm_start)

    user_new = lax.map(solve_owner, (item_idx, item_conf, user_start.reshape(GROUP_SIZE, USERS_DEV, FACTORS))).reshape(NUM_USERS, FACTORS)
    user_bf = user_new.astype(jnp.bfloat16).astype(jnp.float32)
    gram_users = jnp.dot(user_bf.T, user_bf, precision=FULL_PREC) + reg_eye
    user_base = (jnp.arange(GROUP_SIZE) * USERS_DEV).reshape(GROUP_SIZE, 1, 1, 1)
    user_idx = (by_user_idx.reshape(GROUP_SIZE, GROUP_SIZE, ITEMS_DEV, ITEM_SLOTS) + user_base).transpose(1, 0, 2, 3)
    user_conf = by_user_conf.reshape(GROUP_SIZE, GROUP_SIZE, ITEMS_DEV, ITEM_SLOTS).transpose(1, 0, 2, 3)

    def solve_shard(shard_args):
        global_idx, conf_blk, warm_start = shard_args
        return solve_rows(user_bf[global_idx], conf_blk, gram_users, warm_start)

    item_new = lax.map(solve_shard, (user_idx, user_conf, item_factors.reshape(GROUP_SIZE, ITEMS_DEV, FACTORS))).reshape(NUM_ITEMS, FACTORS)
    return (user_new, item_new)
```

```python
import functools

import jax
import jax.numpy as jnp
from jax import lax
from jax.experimental import pallas as pl
from jax.experimental.pallas import tpu as pltpu
from jax.sharding import PartitionSpec as P


REG_LAMBDA = 0.01
CG_STEPS = 3
F = 64
FX = F + 16
PITCH = F + 8
LN = 128
G = 128
PAY = 48
EMPTY = 2048
PACK = 4096
F32 = jnp.float32
BF16 = jnp.bfloat16
I16 = jnp.int16
I32 = jnp.int32


def iota(shape, dim, dtype=I32):
    return lax.broadcasted_iota(dtype, shape, dim)


def take(x, ind, axis):
    other = 1 - axis
    dims = lax.GatherDimensionNumbers(
        offset_dims=(), collapsed_slice_dims=(axis,), start_index_map=(axis,),
        operand_batching_dims=(other,), start_indices_batching_dims=(other,))
    return lax.gather(x, ind[..., None], dims, slice_sizes=(1, 1),
                      mode=lax.GatherScatterMode.PROMISE_IN_BOUNDS)


def dot_nt(a, b):
    return lax.dot_general(a, b, (((1,), (1,)), ((), ())), preferred_element_type=F32)


def fold(gram):
    return jnp.concatenate([gram[:F // 2], gram[F // 2:]], axis=1)


def unfold(gram):
    return jnp.concatenate([gram[:, :F], gram[:, F:]], axis=0)


def table_kernel(x_ref, tab_ref, gram_ref):
    x = x_ref[...].astype(BF16)
    for h in range(x.shape[1] // LN):
        tab_ref[h] = x[:, h * LN:(h + 1) * LN]
    gram_ref[...] = fold(dot_nt(x, x))


def make_table(x_t):
    n = x_t.shape[1]
    return pl.pallas_call(
        table_kernel,
        out_shape=(jax.ShapeDtypeStruct((n // LN, F, LN), BF16), jax.ShapeDtypeStruct((F // 2, LN), F32)),
        name='table',
    )(x_t)


def code_weight(idx, conf):
    code = jnp.where(conf > 0.0, idx, EMPTY).astype(F32)
    return code, jnp.maximum(conf - 1.0, 0.0)


def user_payload_kernel(me_ref, idx_ref, conf_ref, out_ref):
    skew = me_ref[0] % 16
    row, lane = iota((8, LN), 0), iota((8, LN), 1)
    first = (lane - 16 * row) & 127
    second = ((lane >> 4) - row) & 7
    third = ((lane ^ skew) + 16 * row) & 127

    def arrange(x):
        return take(take(take(x, first, 1), second, 0), third, 1)

    def place(dest, _):
        codes = []
        for q in range(4):
            cols = pl.ds(pl.multiple_of(dest * 512 + q * LN, LN), LN)
            code, weight = code_weight(idx_ref[:, cols], conf_ref[:, cols])
            out_ref[dest, pl.ds(q * 8, 8), :] = arrange(weight)
            codes.append(arrange(code))
        for q in range(2):
            out_ref[dest, pl.ds(32 + q * 8, 8), :] = codes[q] + PACK * codes[q + 2]
        return 0

    lax.fori_loop(0, out_ref.shape[0], place, 0, unroll=min(8, out_ref.shape[0]))


def user_payload(me, idx_t, conf_t, dests):
    step = min(32, dests)
    spec = pl.BlockSpec((8, step * 512), lambda i: (0, i))
    return pl.pallas_call(
        user_payload_kernel,
        grid=(dests // step,),
        in_specs=[pl.BlockSpec(memory_space=pltpu.SMEM), spec, spec],
        out_specs=pl.BlockSpec((step, PAY, LN), lambda i: (i, 0, 0)),
        out_shape=jax.ShapeDtypeStruct((dests, PAY, LN), F32),
        name='user_payload',
    )(me, idx_t, conf_t)


def item_payload_kernel(me_ref, idx_ref, conf_ref, out_ref):
    skew = me_ref[0] % 64
    lane = iota((8, LN), 1)
    pattern = lane ^ skew
    low = lane < 64

    def halves(x0, x1):
        a = jnp.where(low, x0, pltpu.roll(x1, 64, 1))
        b = jnp.where(low, pltpu.roll(x0, 64, 1), x1)
        return take(a, pattern, 1), take(b, pattern, 1)

    def place(dest, _):
        for q in range(2):
            base = dest * 32 + q * 16
            rows = [pl.ds(base + j, 8, stride=2) for j in range(2)]
            pairs = [code_weight(idx_ref[r, :], conf_ref[r, :]) for r in rows]
            code_a, code_b = halves(pairs[0][0], pairs[1][0])
            weight_a, weight_b = halves(pairs[0][1], pairs[1][1])
            out_ref[dest, pl.ds(q * 8, 8), :] = weight_a
            out_ref[dest, pl.ds(16 + q * 8, 8), :] = weight_b
            out_ref[dest, pl.ds(32 + q * 8, 8), :] = code_a + PACK * code_b
        return 0

    lax.fori_loop(0, out_ref.shape[0], place, 0, unroll=min(8, out_ref.shape[0]))


def item_payload(me, idx_rows, conf_rows, dests):
    step = min(32, dests)
    spec = pl.BlockSpec((step * 32, LN), lambda i: (i, 0))
    return pl.pallas_call(
        item_payload_kernel,
        grid=(dests // step,),
        in_specs=[pl.BlockSpec(memory_space=pltpu.SMEM), spec, spec],
        out_specs=pl.BlockSpec((step, PAY, LN), lambda i: (i, 0, 0)),
        out_shape=jax.ShapeDtypeStruct((dests, PAY, LN), F32),
        name='item_payload',
    )(me, idx_rows, conf_rows)


ORDERS = ((2, 1, 0), (1, 0, 2), (0, 2, 1))
STRIDES = (32, 8, 2)
RING = 4


def gather_kernel(streams, *refs):
    arrays = len({s[0] for s in streams})
    ins, outs = refs[:arrays], refs[arrays:2 * arrays]
    send, recv, pass_send, pass_recv, local = refs[2 * arrays:]
    me = lax.axis_index('g')
    core = me % 2
    here = [me // stride % RING for stride in STRIDES]
    partner = me + 1 - 2 * core

    def beside(dim, delta):
        return me + ((here[dim] + delta + RING) % RING - here[dim]) * STRIDES[dim]

    barrier = pltpu.get_barrier_semaphore()
    peers = [beside(dim, delta) for dim in range(3) for delta in (1, -1)] + [partner]
    for peer in peers:
        pl.semaphore_signal(barrier, inc=1, device_id={'g': peer}, device_id_type=pl.DeviceIdType.MESH)
    pl.semaphore_wait(barrier, len(peers))

    def region(s, phase, dim, delta, half):
        which, first, rows = streams[s][:3]
        order = ORDERS[streams[s][3]]
        index = []
        for d in range(3):
            if d in order[:phase]:
                index.append(pl.ds(0, RING))
            else:
                index.append((here[d] + delta + RING) % RING if d == dim else here[d])
        if half is not None:
            rows = rows // 2
            first = first + half * rows
        return outs[which].at[(*index, core, pl.ds(first, rows), slice(None))]

    def remote(src, dst, sems, index, peer):
        return pltpu.make_async_remote_copy(
            src_ref=src, dst_ref=dst, send_sem=sems[0].at[index], recv_sem=sems[1].at[index],
            device_id={'g': peer}, device_id_type=pl.DeviceIdType.MESH)

    passed = []

    def pass_on(src, dst, s, slot):
        copy = remote(src, dst, (pass_send, pass_recv), 13 * s + slot, partner)
        copy.start()
        passed.append(copy)

    own, kept = [], []
    for s, (which, first, rows, _) in enumerate(streams):
        src = ins[which].at[pl.ds(first, rows), :]
        own.append(src)
        copy = pltpu.make_async_copy(src, region(s, 0, 0, 0, None), local.at[s])
        copy.start()
        kept.append(copy)
    sent = []
    for phase in range(3):
        across = {}
        for s in range(len(streams)):
            dim = ORDERS[streams[s][3]][phase]
            for way, delta in enumerate((1, -1)):
                mine = region(s, phase, dim, 0, None)
                src = own[s] if phase == 0 else mine
                across[s, way] = remote(src, mine, (send, recv), ((s * 3 + phase) * 2 + 0) * 2 + way, beside(dim, delta))
                across[s, way].start()
        if phase == 0:
            for s in range(len(streams)):
                pass_on(own[s], region(s, 0, 0, 0, None), s, 0)
        further = {}
        for s in range(len(streams)):
            dim = ORDERS[streams[s][3]][phase]
            for way, delta in enumerate((1, -1)):
                across[s, way].wait_recv()
                half = region(s, phase, dim, -delta, way)
                further[s, way] = remote(half, half, (send, recv), ((s * 3 + phase) * 2 + 1) * 2 + way, beside(dim, delta))
                further[s, way].start()
                whole = region(s, phase, dim, -delta, None)
                pass_on(whole, whole, s, 1 + 4 * phase + way)
        for s in range(len(streams)):
            dim = ORDERS[streams[s][3]][phase]
            for way in range(2):
                further[s, way].wait_recv()
                half = region(s, phase, dim, 2, way)
                pass_on(half, half, s, 3 + 4 * phase + way)
        if phase == 0:
            for copy in kept:
                copy.wait()
        sent += list(across.values()) + list(further.values())
    for copy in sent:
        copy.wait_send()
    for copy in passed:
        copy.wait_send()
    for copy in passed:
        copy.wait_recv()


def gather_all(table, gram, collective_id):
    rows = table.shape[0]
    third = rows // 3 // 32 * 32
    sizes = (rows - 2 * third, third, third)
    streams, first = [], 0
    for n, size in enumerate(sizes):
        streams.append((0, first, size, n))
        first += size
    streams.append((1, 0, gram.shape[0], 0))
    count = len(streams)
    any_spec = pl.BlockSpec(memory_space=pl.ANY)
    tables, grams = pl.pallas_call(
        functools.partial(gather_kernel, tuple(streams)),
        in_specs=[pl.BlockSpec(memory_space=pltpu.VMEM)] * 2,
        out_specs=[any_spec] * 2,
        out_shape=[jax.ShapeDtypeStruct((RING, RING, RING, 2, *x.shape), x.dtype) for x in (table, gram)],
        scratch_shapes=[pltpu.SemaphoreType.DMA((12 * count,)), pltpu.SemaphoreType.DMA((12 * count,)),
                        pltpu.SemaphoreType.DMA((13 * count,)), pltpu.SemaphoreType.DMA((13 * count,)),
                        pltpu.SemaphoreType.DMA((count,))],
        compiler_params=pltpu.CompilerParams(collective_id=collective_id, has_side_effects=True),
        name='gather_all',
    )(table, gram)
    return tables.reshape(G, rows, LN), grams.reshape(-1, LN)


def half_kernel(slots, blocks, pair, lanes_of, emit, tab_hbm, pay_hbm, gram_ref, x0_ref, *refs):
    if emit:
        out_ref, tab_ref, gout_ref = refs[:3]
        refs = refs[3:]
    else:
        out_ref = refs[0]
        refs = refs[1:]
    tab, pay, ids, yg, yu_a, yu_b, wu_a, wu_b, a_scr, at_scr, p_scr, s_scr, sems = refs
    per = LN // slots
    chunks = G // per
    groups = LN // per
    steps = blocks * groups // pair
    turns = groups // pair
    heads = tab.shape[1]

    pay_copy = pltpu.make_async_copy(pay_hbm, pay, sems.at[8])
    pay_copy.start()

    def tab_copy(i):
        return pltpu.make_async_copy(tab_hbm.at[pl.ds(16 * i, 16)], tab.at[pl.ds(16 * i, 16)], sems.at[i])

    for i in range(8):
        tab_copy(i).start()
    ids[...] = iota((2 * LN, LN), 0, I16)
    pay_copy.wait()

    lane16 = iota((16, LN), 1, I16)
    lane = iota((8, LN), 1)
    row = iota((8, LN), 0)

    def add_gram(d, acc):
        return acc + gram_ref[pl.ds(pl.multiple_of(d * (F // 2), F // 2), F // 2), :]

    gram = lax.fori_loop(0, G, add_gram, jnp.zeros((F // 2, LN), F32), unroll=8)
    gpad = jnp.concatenate([unfold(gram), jnp.zeros((16, F), F32)], axis=0)
    gpad = jnp.concatenate([gpad, jnp.zeros((FX, 16), F32)], axis=1)
    rr, cc = iota((FX, FX), 0), iota((FX, FX), 1)
    gpad = gpad + jnp.where((rr == cc) & (rr < F), REG_LAMBDA, 0.0)

    def pay_row(t):
        if slots == 8:
            return t, 32 + t % 16, 12 * (t // 16)
        return (t % 2) * 16 + t // 2, 32 + t // 2, 12 * (t % 2)

    def spread_weights(t, wu, q):
        wrow = pay_row(t)[0]
        for c in range(chunks):
            tiles = []
            for v in range(per // 8):
                start = (per * c + 8 * v) * PAY + wrow
                tiles.append(pay[pl.ds(start, 8, stride=PAY), :])
            for bit in (1, 2, 4):
                hit = (lane & bit) != 0
                up = (row & bit) != 0
                for v in range(len(tiles)):
                    x = tiles[v]
                    if bit == 4:
                        other = pltpu.roll(x, 4, 0)
                    else:
                        other = jnp.where(up, pltpu.roll(x, bit, 0), pltpu.roll(x, 8 - bit, 0))
                    tiles[v] = jnp.where(hit, other, x)
            bit = 8
            while bit < per:
                hit = (lane & bit) != 0
                tiles = [jnp.where(hit, tiles[v ^ (bit // 8)], tiles[v]) for v in range(len(tiles))]
                bit *= 2
            for v in range(len(tiles)):
                wu[c, pl.ds(per * q + 8 * v, 8), :] = tiles[v]

    def exchange(xs, low_bit):
        bit, n = 1, len(xs)
        while bit < n:
            hit = (lane16 & I16(bit * low_bit)) != I16(0)
            xs = [jnp.where(hit, xs[a ^ bit], xs[a]) for a in range(n)]
            bit *= 2
        return xs

    def regroup(i, yu):
        for q in range(pair):
            for k in range(4):
                rows = pl.ds(16 * k, 16)
                xs = exchange([yg[q, d, rows, :] for d in range(16)], 1)
                for a in range(16):
                    if slots == 8:
                        yu[16 * q + a, i, rows, :] = xs[a]
                    else:
                        yu[64 * q + (i % 4) * 16 + a, i // 4, rows, :] = xs[a]

    ones = jnp.ones((16, LN * chunks), BF16)

    def form(y_parts, wu, u, at):
        vs = []
        for c in range(chunks):
            w = wu[c, pl.ds(u, 1), :]
            vs.append((y_parts[c].astype(F32) * w).astype(BF16))
        y = jnp.concatenate([jnp.concatenate(y_parts, axis=1), ones], axis=0)
        v = jnp.concatenate([jnp.concatenate(vs, axis=1), ones], axis=0)
        a_scr[pl.ds(at * PITCH, PITCH), pl.ds(0, FX)] = (dot_nt(y, v) + gpad)[:PITCH]

    def form_rows(t, i, yu, wu):
        done = jnp.maximum(t - 1, 0)
        first = done // turns % 2 * LN + done % turns * (per * pair)
        if slots == 8:
            for e in range(2 * pair):
                u = 2 * pair * i + e
                form([yu[u, c] for c in range(chunks)], wu, u, first + u)
        else:
            for q in range(pair):
                for e in range(2):
                    r = 64 * q + 2 * i + e
                    parts = []
                    for c in range(chunks):
                        by_k = [exchange([yu[r + 16 * m, c, pl.ds(16 * k, 16), :] for m in range(4)], 16)
                                for k in range(4)]
                        parts.append([jnp.concatenate([by_k[k][m] for k in range(4)], axis=0) for m in range(4)])
                    for m in range(4):
                        form([parts[c][m] for c in range(chunks)], wu, r + 16 * m, first + r + 16 * m)

    def codes(t, d, q):
        _, crow, shift = pay_row(pair * t + q)
        packed = pay[pl.ds(d * PAY + crow, 1), :].astype(I32)
        return (packed >> shift) & (PACK - 1)

    def by_lanes(t, d, dd, q):
        code = jnp.broadcast_to(codes(t, d, q), (F, LN)).astype(I16)
        low = code & I16(LN - 1)
        head = code >> I16(7)
        acc = jnp.zeros((F, LN), BF16)
        for h in range(heads):
            acc = jnp.where(head == I16(h), take(tab[d, h], low, 1), acc)
        yg[q, dd] = acc

    def by_matmul(t, d, dd):
        hots, halves = [], []
        for q in range(2):
            code = codes(t, d, q)
            low = (jnp.broadcast_to(code, (2 * LN, LN)) & (2 * LN - 1)).astype(I16)
            hots.append(jnp.where(low == ids[...], jnp.ones((2 * LN, LN), BF16), jnp.zeros((2 * LN, LN), BF16)))
            halves.append(jnp.broadcast_to(code, (F, LN)) >> 8)
        table = jnp.concatenate([jnp.concatenate([tab[d, 2 * h], tab[d, 2 * h + 1]], axis=1)
                                 for h in range(heads // 2)], axis=0)
        found = jnp.dot(table, jnp.concatenate(hots, axis=1), preferred_element_type=F32)
        for q in range(2):
            acc = jnp.zeros((F, LN), F32)
            for h in range(heads // 2):
                acc = jnp.where(halves[q] == h, found[h * F:(h + 1) * F, q * LN:(q + 1) * LN], acc)
            yg[q, dd] = acc.astype(BF16)

    def lookup(t, i):
        turn = 0
        for dd in range(16):
            d = 16 * i + dd
            turn += lanes_of
            if turn >= 16:
                turn -= 16
                for q in range(pair):
                    by_lanes(t, d, dd, q)
            else:
                by_matmul(t, d, dd)

    def flip(block, b):
        m = a_scr[pl.ds(block % 2 * (LN * PITCH) + b, LN, stride=PITCH), :].T
        at_scr[b] = m[:F]
        s_scr[pl.ds(b, 1), :] = m[F:F + 1]

    def flip_all(block):
        def four(b4, _):
            for e in range(4):
                flip(block, 4 * b4 + e)
            return 0

        lax.fori_loop(0, F // 4, four, 0)

    def solve(block):
        rhs = a_scr[pl.ds(block % 2 * (LN * PITCH) + F, LN, stride=PITCH), :].T[:F] + s_scr[...]
        x = x0_ref[:, pl.ds(pl.multiple_of(block * LN, LN), LN)]

        def apply_mat(vec):
            p_scr[...] = vec

            def add(b, acc):
                return acc + at_scr[b] * p_scr[pl.ds(b, 1), :]

            return lax.fori_loop(0, F, add, jnp.zeros((F, LN), F32), unroll=8)

        res = rhs - apply_mat(x)
        direction = res
        res_sq = jnp.sum(res * res, axis=0, keepdims=True)
        for step in range(CG_STEPS):
            q = apply_mat(direction)
            length = res_sq / jnp.sum(direction * q, axis=0, keepdims=True)
            x = x + length * direction
            if step + 1 < CG_STEPS:
                res = res - length * q
                new_sq = jnp.sum(res * res, axis=0, keepdims=True)
                direction = res + (new_sq / res_sq) * direction
                res_sq = new_sq
        out_ref[:, pl.ds(pl.multiple_of(block * LN, LN), LN)] = x
        if emit:
            xb = x.astype(BF16)
            tab_ref[block] = xb
            gout_ref[...] += fold(dot_nt(xb, xb))

    if emit:
        gout_ref[...] = jnp.zeros((F // 2, LN), F32)

    def step_pass(t, parts, yu, wu, yu_last, wu_last):
        now = jnp.minimum(t, steps - 1)
        done = jnp.maximum(t - 1, 0)
        before = jnp.maximum(done // turns - 1, 0)
        for q in range(pair):
            spread_weights(pair * now + q, wu, q)

        def inner(i, _):
            @pl.when(t == 0)
            def _():
                tab_copy(i).wait()

            flips = F // (8 * turns)
            for e in range(flips):
                flip(before, (done % turns * 8 + i) * flips + e)
            form_rows(t, i, yu_last, wu_last)
            regroup((i + 7) % 8, yu)
            lookup(now, i)
            return 0

        lax.fori_loop(0, parts, inner, 0)
        regroup(7, yu)

        @pl.when((t >= turns + 1) & (t <= steps) & (t % turns == 0))
        def _():
            solve(t // turns - 2)

    def two_steps(t2, _):
        step_pass(2 * t2, 8, yu_a, wu_a, yu_b, wu_b)
        step_pass(2 * t2 + 1, jnp.where(2 * t2 + 1 <= steps, 8, 0), yu_b, wu_b, yu_a, wu_a)
        return 0

    lax.fori_loop(0, steps // 2 + 1, two_steps, 0)
    flip_all(blocks - 1)
    solve(blocks - 1)


def half_step(slots, emit, pair, lanes_of, tables, payload, gram, x0_t):
    n = x0_t.shape[1]
    heads = tables.shape[1]
    per = LN // slots
    chunks = G // per
    out_shape = [jax.ShapeDtypeStruct((F, n), F32)]
    if emit:
        out_shape += [jax.ShapeDtypeStruct((n // LN, F, LN), BF16), jax.ShapeDtypeStruct((F // 2, LN), F32)]
    vmem = pl.BlockSpec(memory_space=pltpu.VMEM)
    return pl.pallas_call(
        functools.partial(half_kernel, slots, n // LN, pair, lanes_of, emit),
        in_specs=[pl.BlockSpec(memory_space=pl.ANY), pl.BlockSpec(memory_space=pl.ANY), vmem, vmem],
        out_specs=[vmem] * len(out_shape),
        out_shape=out_shape,
        scratch_shapes=[
            pltpu.VMEM((G, heads, F, LN), BF16),
            pltpu.VMEM((G * PAY, LN), F32),
            pltpu.VMEM((2 * LN, LN), I16),
            pltpu.VMEM((pair, 16, F, LN), BF16),
            pltpu.VMEM((pair * per, chunks, F, LN), BF16),
            pltpu.VMEM((pair * per, chunks, F, LN), BF16),
            pltpu.VMEM((chunks, pair * per, LN), F32),
            pltpu.VMEM((chunks, pair * per, LN), F32),
            pltpu.VMEM((2 * LN * PITCH, LN), F32),
            pltpu.VMEM((F, F, LN), F32),
            pltpu.VMEM((F, LN), F32),
            pltpu.VMEM((F, LN), F32),
            pltpu.SemaphoreType.DMA((9,)),
        ],
        compiler_params=pltpu.CompilerParams(vmem_limit_bytes=62 * 1024 * 1024),
        cost_estimate=pl.CostEstimate(flops=10 ** 11, bytes_accessed=2 ** 25, transcendentals=0),
        name='half_step',
    )(tables, payload, gram, x0_t)


def solution(mesh):
    part_spec = P(('tables', 'g'), None)
    slot_spec = P(('tables', 'g'), None, None)

    def local_sweep(item_block, start_block, item_idx, item_conf, user_idx, user_conf):
        me = lax.axis_index('g').astype(I32).reshape(1)
        item_t = item_block.T
        table, gram_part = make_table(item_t)
        payload = user_payload(me, item_idx[0].T, item_conf[0].T, G)
        payload = lax.all_to_all(payload, 'g', 0, 0, tiled=True)

        def as_rows(x):
            return x[0].reshape(-1, LN, 2).transpose(0, 2, 1).reshape(-1, LN)

        late = item_payload(me, as_rows(user_idx), as_rows(user_conf), G)
        late = lax.all_to_all(late, 'g', 0, 0, tiled=True)

        tables, gram_items = gather_all(table.reshape(-1, LN), gram_part, 0)
        tables = tables.reshape(G, -1, F, LN)
        user_t, user_table, gram_part = half_step(8, True, 2, 6, tables, payload.reshape(G * PAY, LN),
                                                  gram_items, start_block.T)
        user_tables, gram_users = gather_all(user_table.reshape(-1, LN), gram_part, 1)
        user_tables = user_tables.reshape(G, -1, F, LN)
        item_new = half_step(2, False, 2, 8, user_tables, late.reshape(G * PAY, LN), gram_users, item_t)[0]
        return user_t.T, item_new.T

    return jax.shard_map(local_sweep, mesh=mesh,
                         in_specs=(part_spec, part_spec, slot_spec, slot_spec, slot_spec, slot_spec),
                         out_specs=(part_spec, part_spec), check_vma=False)
```

```python
import functools

import jax
import jax.numpy as jnp
from jax import lax
from jax.experimental import pallas as pl
from jax.experimental.pallas import tpu as pltpu
from jax.sharding import PartitionSpec as P


REG_LAMBDA = 0.01
CG_STEPS = 3
F = 64
FX = F + 16
PITCH = F + 8
LN = 128
G = 128
PAY = 48
EMPTY = 2048
PACK = 4096
F32 = jnp.float32
BF16 = jnp.bfloat16
I16 = jnp.int16
I32 = jnp.int32


def iota(shape, dim, dtype=I32):
    return lax.broadcasted_iota(dtype, shape, dim)


def take(x, ind, axis):
    other = 1 - axis
    dims = lax.GatherDimensionNumbers(
        offset_dims=(), collapsed_slice_dims=(axis,), start_index_map=(axis,),
        operand_batching_dims=(other,), start_indices_batching_dims=(other,))
    return lax.gather(x, ind[..., None], dims, slice_sizes=(1, 1),
                      mode=lax.GatherScatterMode.PROMISE_IN_BOUNDS)


def dot_nt(a, b):
    return lax.dot_general(a, b, (((1,), (1,)), ((), ())), preferred_element_type=F32)


def fold(gram):
    return jnp.concatenate([gram[:F // 2], gram[F // 2:]], axis=1)


def unfold(gram):
    return jnp.concatenate([gram[:, :F], gram[:, F:]], axis=0)


def table_kernel(x_ref, tab_ref, gram_ref):
    x = x_ref[...].astype(BF16)
    for h in range(x.shape[1] // LN):
        tab_ref[h] = x[:, h * LN:(h + 1) * LN]
    gram_ref[...] = fold(dot_nt(x, x))


def make_table(x_t):
    n = x_t.shape[1]
    return pl.pallas_call(
        table_kernel,
        out_shape=(jax.ShapeDtypeStruct((n // LN, F, LN), BF16), jax.ShapeDtypeStruct((F // 2, LN), F32)),
        name='table',
    )(x_t)


def code_weight(idx, conf):
    code = jnp.where(conf > 0.0, idx, EMPTY).astype(F32)
    return code, jnp.maximum(conf - 1.0, 0.0)


def user_payload_kernel(me_ref, idx_ref, conf_ref, out_ref):
    skew = me_ref[0] % 16
    row, lane = iota((8, LN), 0), iota((8, LN), 1)
    first = (lane - 16 * row) & 127
    second = ((lane >> 4) - row) & 7
    third = ((lane ^ skew) + 16 * row) & 127

    def arrange(x):
        return take(take(take(x, first, 1), second, 0), third, 1)

    def place(dest, _):
        codes = []
        for q in range(4):
            cols = pl.ds(pl.multiple_of(dest * 512 + q * LN, LN), LN)
            code, weight = code_weight(idx_ref[:, cols], conf_ref[:, cols])
            out_ref[dest, pl.ds(q * 8, 8), :] = arrange(weight)
            codes.append(arrange(code))
        for q in range(2):
            out_ref[dest, pl.ds(32 + q * 8, 8), :] = codes[q] + PACK * codes[q + 2]
        return 0

    lax.fori_loop(0, out_ref.shape[0], place, 0, unroll=min(8, out_ref.shape[0]))


def user_payload(me, idx_t, conf_t, dests):
    step = min(32, dests)
    spec = pl.BlockSpec((8, step * 512), lambda i: (0, i))
    return pl.pallas_call(
        user_payload_kernel,
        grid=(dests // step,),
        in_specs=[pl.BlockSpec(memory_space=pltpu.SMEM), spec, spec],
        out_specs=pl.BlockSpec((step, PAY, LN), lambda i: (i, 0, 0)),
        out_shape=jax.ShapeDtypeStruct((dests, PAY, LN), F32),
        name='user_payload',
    )(me, idx_t, conf_t)


def arrange_items(me, idx_ref, conf_ref, out_ref):
    skew = me % 64
    lane = iota((8, LN), 1)
    pattern = lane ^ skew
    low = lane < 64

    def halves(x0, x1):
        a = jnp.where(low, x0, pltpu.roll(x1, 64, 1))
        b = jnp.where(low, pltpu.roll(x0, 64, 1), x1)
        return take(a, pattern, 1), take(b, pattern, 1)

    def place(dest, _):
        for q in range(2):
            base = dest * 32 + q * 16
            rows = [pl.ds(base + j, 8, stride=2) for j in range(2)]
            pairs = [code_weight(idx_ref[r, :], conf_ref[r, :]) for r in rows]
            code_a, code_b = halves(pairs[0][0], pairs[1][0])
            weight_a, weight_b = halves(pairs[0][1], pairs[1][1])
            out_ref[dest, pl.ds(q * 8, 8), :] = weight_a
            out_ref[dest, pl.ds(16 + q * 8, 8), :] = weight_b
            out_ref[dest, pl.ds(32 + q * 8, 8), :] = code_a + PACK * code_b
        return 0

    lax.fori_loop(0, out_ref.shape[0], place, 0, unroll=min(8, out_ref.shape[0]))


ORDERS = ((2, 1, 0), (1, 0, 2), (0, 2, 1))
STRIDES = (32, 8, 2)
RING = 4


def gather_kernel(streams, beside_work, *refs):
    if beside_work:
        table, gram, idx_hbm, conf_hbm, *outs, pay_hbm, send, recv, pass_send, pass_recv, local, idx, conf, pay, work = refs
        loads = [pltpu.make_async_copy(idx_hbm, idx, work.at[0]), pltpu.make_async_copy(conf_hbm, conf, work.at[1])]
        for copy in loads:
            copy.start()
    else:
        table, gram, *outs, send, recv, pass_send, pass_recv, local = refs
    ins = (table, gram)
    me = lax.axis_index('g')
    core = me % 2
    here = [me // stride % RING for stride in STRIDES]
    partner = me + 1 - 2 * core

    def beside(dim, delta):
        return me + ((here[dim] + delta + RING) % RING - here[dim]) * STRIDES[dim]

    barrier = pltpu.get_barrier_semaphore()
    peers = [beside(dim, delta) for dim in range(3) for delta in (1, -1)] + [partner]
    for peer in peers:
        pl.semaphore_signal(barrier, inc=1, device_id={'g': peer}, device_id_type=pl.DeviceIdType.MESH)
    pl.semaphore_wait(barrier, len(peers))

    def region(s, phase, dim, delta, half):
        which, first, rows = streams[s][:3]
        order = ORDERS[streams[s][3]]
        index = []
        for d in range(3):
            if d in order[:phase]:
                index.append(pl.ds(0, RING))
            else:
                index.append((here[d] + delta + RING) % RING if d == dim else here[d])
        if half is not None:
            rows = rows // 2
            first = first + half * rows
        return outs[which].at[(*index, core, pl.ds(first, rows), slice(None))]

    def remote(src, dst, sems, index, peer):
        return pltpu.make_async_remote_copy(
            src_ref=src, dst_ref=dst, send_sem=sems[0].at[index], recv_sem=sems[1].at[index],
            device_id={'g': peer}, device_id_type=pl.DeviceIdType.MESH)

    passed = []

    def pass_on(src, dst, s, slot):
        copy = remote(src, dst, (pass_send, pass_recv), 13 * s + slot, partner)
        copy.start()
        passed.append(copy)

    count = len(streams)
    own, kept = [], []
    for s, (which, first, rows, _) in enumerate(streams):
        src = ins[which].at[pl.ds(first, rows), :]
        own.append(src)
        copy = pltpu.make_async_copy(src, region(s, 0, 0, 0, None), local.at[s])
        copy.start()
        kept.append(copy)
    sent, across, further = [], {}, {}

    def start_across(s, phase):
        dim = ORDERS[streams[s][3]][phase]
        for way, delta in enumerate((1, -1)):
            mine = region(s, phase, dim, 0, None)
            src = own[s] if phase == 0 else mine
            across[s, way] = remote(src, mine, (send, recv), ((s * 3 + phase) * 2 + 0) * 2 + way, beside(dim, delta))
            across[s, way].start()
            sent.append(across[s, way])

    def start_further(s, phase):
        dim = ORDERS[streams[s][3]][phase]
        for way, delta in enumerate((1, -1)):
            across[s, way].wait_recv()
            half = region(s, phase, dim, -delta, way)
            further[s, way] = remote(half, half, (send, recv), ((s * 3 + phase) * 2 + 1) * 2 + way, beside(dim, delta))
            further[s, way].start()
            sent.append(further[s, way])
        for way, delta in enumerate((1, -1)):
            whole = region(s, phase, dim, -delta, None)
            pass_on(whole, whole, s, 1 + 4 * phase + way)

    def finish(s, phase):
        dim = ORDERS[streams[s][3]][phase]
        for way in range(2):
            further[s, way].wait_recv()
        if phase == 0:
            kept[s].wait()
        if phase < 2:
            start_across(s, phase + 1)
        for way in range(2):
            half = region(s, phase, dim, 2, way)
            pass_on(half, half, s, 3 + 4 * phase + way)

    for s in range(count):
        start_across(s, 0)
    for s in range(count):
        pass_on(own[s], region(s, 0, 0, 0, None), s, 0)
    for phase in range(3):
        for s in range(count):
            start_further(s, phase)
        for s in range(count):
            finish(s, phase)
        if phase == 1 and beside_work:
            for copy in loads:
                copy.wait()
            arrange_items(me, idx, conf, pay)
            store = pltpu.make_async_copy(pay, pay_hbm, work.at[2])
            store.start()
    if beside_work:
        store.wait()
    for copy in sent:
        copy.wait_send()
    for copy in passed:
        copy.wait_send()
    for copy in passed:
        copy.wait_recv()


def gather_all(table, gram, collective_id, slot_rows=()):
    rows = table.shape[0]
    units = rows // 16
    large = -(-units // 6)
    sizes = (large, large, (units - 4 * large) // 2) * 2
    streams, first = [(1, 0, gram.shape[0], 2)], 0
    for n, size in enumerate(sizes):
        streams.append((0, first, 16 * size, n % 3))
        first += 16 * size
    count = len(streams)
    any_spec = pl.BlockSpec(memory_space=pl.ANY)
    out_shape = [jax.ShapeDtypeStruct((RING, RING, RING, 2, *x.shape), x.dtype) for x in (table, gram)]
    scratch = [pltpu.SemaphoreType.DMA((12 * count,)), pltpu.SemaphoreType.DMA((12 * count,)),
               pltpu.SemaphoreType.DMA((13 * count,)), pltpu.SemaphoreType.DMA((13 * count,)),
               pltpu.SemaphoreType.DMA((count,))]
    if slot_rows:
        dests = slot_rows[0].shape[0] // 32
        out_shape.append(jax.ShapeDtypeStruct((dests, PAY, LN), F32))
        scratch += [pltpu.VMEM(x.shape, x.dtype) for x in slot_rows]
        scratch += [pltpu.VMEM((dests, PAY, LN), F32), pltpu.SemaphoreType.DMA((3,))]
    tables, grams, *payload = pl.pallas_call(
        functools.partial(gather_kernel, tuple(streams), bool(slot_rows)),
        in_specs=[pl.BlockSpec(memory_space=pltpu.VMEM)] * 2 + [any_spec] * len(slot_rows),
        out_specs=[any_spec] * len(out_shape),
        out_shape=out_shape,
        scratch_shapes=scratch,
        compiler_params=pltpu.CompilerParams(collective_id=collective_id, has_side_effects=True),
        name='gather_all',
    )(table, gram, *slot_rows)
    return tables.reshape(G, rows, LN), grams.reshape(-1, LN), *payload


def half_kernel(slots, blocks, pair, lanes_of, emit, tab_hbm, pay_hbm, gram_ref, x0_ref, *refs):
    if emit:
        out_ref, tab_ref, gout_ref = refs[:3]
        refs = refs[3:]
    else:
        out_ref = refs[0]
        refs = refs[1:]
    tab, pay, ids, yg, yu_a, yu_b, wu_a, wu_b, a_scr, at_scr, p_scr, s_scr, sems = refs
    per = LN // slots
    chunks = G // per
    groups = LN // per
    steps = blocks * groups // pair
    turns = groups // pair
    heads = tab.shape[1]

    pay_copy = pltpu.make_async_copy(pay_hbm, pay, sems.at[8])
    pay_copy.start()

    def tab_copy(i):
        return pltpu.make_async_copy(tab_hbm.at[pl.ds(16 * i, 16)], tab.at[pl.ds(16 * i, 16)], sems.at[i])

    for i in range(8):
        tab_copy(i).start()
    ids[...] = iota((2 * LN, LN), 0, I16)
    pay_copy.wait()

    lane16 = iota((16, LN), 1, I16)
    lane = iota((8, LN), 1)
    row = iota((8, LN), 0)

    def add_gram(d, acc):
        return acc + gram_ref[pl.ds(pl.multiple_of(d * (F // 2), F // 2), F // 2), :]

    gram = lax.fori_loop(0, G, add_gram, jnp.zeros((F // 2, LN), F32), unroll=8)
    gpad = jnp.concatenate([unfold(gram), jnp.zeros((16, F), F32)], axis=0)
    gpad = jnp.concatenate([gpad, jnp.zeros((FX, 16), F32)], axis=1)
    rr, cc = iota((FX, FX), 0), iota((FX, FX), 1)
    gpad = gpad + jnp.where((rr == cc) & (rr < F), REG_LAMBDA, 0.0)

    def pay_row(t):
        if slots == 8:
            return t, 32 + t % 16, 12 * (t // 16)
        return (t % 2) * 16 + t // 2, 32 + t // 2, 12 * (t % 2)

    def spread_weights(t, wu, q):
        wrow = pay_row(t)[0]
        for c in range(chunks):
            tiles = []
            for v in range(per // 8):
                start = (per * c + 8 * v) * PAY + wrow
                tiles.append(pay[pl.ds(start, 8, stride=PAY), :])
            for bit in (1, 2, 4):
                hit = (lane & bit) != 0
                up = (row & bit) != 0
                for v in range(len(tiles)):
                    x = tiles[v]
                    if bit == 4:
                        other = pltpu.roll(x, 4, 0)
                    else:
                        other = jnp.where(up, pltpu.roll(x, bit, 0), pltpu.roll(x, 8 - bit, 0))
                    tiles[v] = jnp.where(hit, other, x)
            bit = 8
            while bit < per:
                hit = (lane & bit) != 0
                tiles = [jnp.where(hit, tiles[v ^ (bit // 8)], tiles[v]) for v in range(len(tiles))]
                bit *= 2
            for v in range(len(tiles)):
                wu[c, pl.ds(per * q + 8 * v, 8), :] = tiles[v]

    def exchange(xs, low_bit):
        bit, n = 1, len(xs)
        while bit < n:
            hit = (lane16 & I16(bit * low_bit)) != I16(0)
            xs = [jnp.where(hit, xs[a ^ bit], xs[a]) for a in range(n)]
            bit *= 2
        return xs

    def regroup(i, yu):
        for q in range(pair):
            for k in range(4):
                rows = pl.ds(16 * k, 16)
                xs = exchange([yg[q, d, rows, :] for d in range(16)], 1)
                for a in range(16):
                    if slots == 8:
                        yu[16 * q + a, i, rows, :] = xs[a]
                    else:
                        yu[64 * q + (i % 4) * 16 + a, i // 4, rows, :] = xs[a]

    ones = jnp.ones((16, LN * chunks), BF16)

    def form(y_parts, wu, u, at):
        vs = []
        for c in range(chunks):
            w = wu[c, pl.ds(u, 1), :]
            vs.append((y_parts[c].astype(F32) * w).astype(BF16))
        y = jnp.concatenate([jnp.concatenate(y_parts, axis=1), ones], axis=0)
        v = jnp.concatenate([jnp.concatenate(vs, axis=1), ones], axis=0)
        a_scr[pl.ds(at * PITCH, PITCH), pl.ds(0, FX)] = (dot_nt(y, v) + gpad)[:PITCH]

    def form_rows(t, i, yu, wu):
        done = jnp.maximum(t - 1, 0)
        first = done // turns % 2 * LN + done % turns * (per * pair)
        if slots == 8:
            for e in range(2 * pair):
                u = 2 * pair * i + e
                form([yu[u, c] for c in range(chunks)], wu, u, first + u)
        else:
            for q in range(pair):
                for e in range(2):
                    r = 64 * q + 2 * i + e
                    parts = []
                    for c in range(chunks):
                        by_k = [exchange([yu[r + 16 * m, c, pl.ds(16 * k, 16), :] for m in range(4)], 16)
                                for k in range(4)]
                        parts.append([jnp.concatenate([by_k[k][m] for k in range(4)], axis=0) for m in range(4)])
                    for m in range(4):
                        form([parts[c][m] for c in range(chunks)], wu, r + 16 * m, first + r + 16 * m)

    def codes(t, d, q):
        _, crow, shift = pay_row(pair * t + q)
        packed = pay[pl.ds(d * PAY + crow, 1), :].astype(I32)
        return (packed >> shift) & (PACK - 1)

    def by_lanes(t, d, dd, q):
        code = jnp.broadcast_to(codes(t, d, q), (F, LN)).astype(I16)
        low = code & I16(LN - 1)
        head = code >> I16(7)
        acc = jnp.zeros((F, LN), BF16)
        for h in range(heads):
            acc = jnp.where(head == I16(h), take(tab[d, h], low, 1), acc)
        yg[q, dd] = acc

    def by_matmul(t, d, dd):
        hots, halves = [], []
        for q in range(2):
            code = codes(t, d, q)
            low = (jnp.broadcast_to(code, (2 * LN, LN)) & (2 * LN - 1)).astype(I16)
            hots.append(jnp.where(low == ids[...], jnp.ones((2 * LN, LN), BF16), jnp.zeros((2 * LN, LN), BF16)))
            halves.append(jnp.broadcast_to(code, (F, LN)) >> 8)
        table = jnp.concatenate([jnp.concatenate([tab[d, 2 * h], tab[d, 2 * h + 1]], axis=1)
                                 for h in range(heads // 2)], axis=0)
        found = jnp.dot(table, jnp.concatenate(hots, axis=1), preferred_element_type=F32)
        for q in range(2):
            acc = jnp.zeros((F, LN), F32)
            for h in range(heads // 2):
                acc = jnp.where(halves[q] == h, found[h * F:(h + 1) * F, q * LN:(q + 1) * LN], acc)
            yg[q, dd] = acc.astype(BF16)

    def lookup(t, i):
        turn = 0
        for dd in range(16):
            d = 16 * i + dd
            turn += lanes_of
            if turn >= 16:
                turn -= 16
                for q in range(pair):
                    by_lanes(t, d, dd, q)
            else:
                by_matmul(t, d, dd)

    def flip(block, b):
        m = a_scr[pl.ds(block % 2 * (LN * PITCH) + b, LN, stride=PITCH), :].T
        at_scr[b] = m[:F]
        s_scr[pl.ds(b, 1), :] = m[F:F + 1]

    def flip_all(block):
        def four(b4, _):
            for e in range(4):
                flip(block, 4 * b4 + e)
            return 0

        lax.fori_loop(0, F // 4, four, 0)

    def solve(block):
        rhs = a_scr[pl.ds(block % 2 * (LN * PITCH) + F, LN, stride=PITCH), :].T[:F] + s_scr[...]
        x = x0_ref[:, pl.ds(pl.multiple_of(block * LN, LN), LN)]

        def apply_mat(vec):
            p_scr[...] = vec

            def add(b, acc):
                return acc + at_scr[b] * p_scr[pl.ds(b, 1), :]

            return lax.fori_loop(0, F, add, jnp.zeros((F, LN), F32), unroll=8)

        res = rhs - apply_mat(x)
        direction = res
        res_sq = jnp.sum(res * res, axis=0, keepdims=True)
        for step in range(CG_STEPS):
            q = apply_mat(direction)
            length = res_sq / jnp.sum(direction * q, axis=0, keepdims=True)
            x = x + length * direction
            if step + 1 < CG_STEPS:
                res = res - length * q
                new_sq = jnp.sum(res * res, axis=0, keepdims=True)
                direction = res + (new_sq / res_sq) * direction
                res_sq = new_sq
        out_ref[:, pl.ds(pl.multiple_of(block * LN, LN), LN)] = x
        if emit:
            xb = x.astype(BF16)
            tab_ref[block] = xb
            gout_ref[...] += fold(dot_nt(xb, xb))

    if emit:
        gout_ref[...] = jnp.zeros((F // 2, LN), F32)

    def step_pass(t, parts, yu, wu, yu_last, wu_last):
        now = jnp.minimum(t, steps - 1)
        done = jnp.maximum(t - 1, 0)
        before = jnp.maximum(done // turns - 1, 0)
        for q in range(pair):
            spread_weights(pair * now + q, wu, q)

        def inner(i, _):
            @pl.when(t == 0)
            def _():
                tab_copy(i).wait()

            flips = F // (8 * turns)
            for e in range(flips):
                flip(before, (done % turns * 8 + i) * flips + e)
            form_rows(t, i, yu_last, wu_last)
            regroup((i + 7) % 8, yu)
            lookup(now, i)
            return 0

        lax.fori_loop(0, parts, inner, 0)
        regroup(7, yu)

        @pl.when((t >= turns + 1) & (t <= steps) & (t % turns == 0))
        def _():
            solve(t // turns - 2)

    def two_steps(t2, _):
        step_pass(2 * t2, 8, yu_a, wu_a, yu_b, wu_b)
        step_pass(2 * t2 + 1, jnp.where(2 * t2 + 1 <= steps, 8, 0), yu_b, wu_b, yu_a, wu_a)
        return 0

    lax.fori_loop(0, steps // 2 + 1, two_steps, 0)
    flip_all(blocks - 1)
    solve(blocks - 1)


def half_step(slots, emit, pair, lanes_of, tables, payload, gram, x0_t):
    n = x0_t.shape[1]
    heads = tables.shape[1]
    per = LN // slots
    chunks = G // per
    out_shape = [jax.ShapeDtypeStruct((F, n), F32)]
    if emit:
        out_shape += [jax.ShapeDtypeStruct((n // LN, F, LN), BF16), jax.ShapeDtypeStruct((F // 2, LN), F32)]
    vmem = pl.BlockSpec(memory_space=pltpu.VMEM)
    return pl.pallas_call(
        functools.partial(half_kernel, slots, n // LN, pair, lanes_of, emit),
        in_specs=[pl.BlockSpec(memory_space=pl.ANY), pl.BlockSpec(memory_space=pl.ANY), vmem, vmem],
        out_specs=[vmem] * len(out_shape),
        out_shape=out_shape,
        scratch_shapes=[
            pltpu.VMEM((G, heads, F, LN), BF16),
            pltpu.VMEM((G * PAY, LN), F32),
            pltpu.VMEM((2 * LN, LN), I16),
            pltpu.VMEM((pair, 16, F, LN), BF16),
            pltpu.VMEM((pair * per, chunks, F, LN), BF16),
            pltpu.VMEM((pair * per, chunks, F, LN), BF16),
            pltpu.VMEM((chunks, pair * per, LN), F32),
            pltpu.VMEM((chunks, pair * per, LN), F32),
            pltpu.VMEM((2 * LN * PITCH, LN), F32),
            pltpu.VMEM((F, F, LN), F32),
            pltpu.VMEM((F, LN), F32),
            pltpu.VMEM((F, LN), F32),
            pltpu.SemaphoreType.DMA((9,)),
        ],
        compiler_params=pltpu.CompilerParams(vmem_limit_bytes=62 * 1024 * 1024),
        cost_estimate=pl.CostEstimate(flops=10 ** 11, bytes_accessed=2 ** 25, transcendentals=0),
        name='half_step',
    )(tables, payload, gram, x0_t)


def solution(mesh):
    part_spec = P(('tables', 'g'), None)
    slot_spec = P(('tables', 'g'), None, None)

    def local_sweep(item_block, start_block, item_idx, item_conf, user_idx, user_conf):
        me = lax.axis_index('g').astype(I32).reshape(1)
        item_t = item_block.T
        table, gram_part = make_table(item_t)
        payload = user_payload(me, item_idx[0].T, item_conf[0].T, G)
        payload = lax.all_to_all(payload, 'g', 0, 0, tiled=True)

        def as_rows(x):
            return x[0].reshape(-1, LN, 2).transpose(0, 2, 1).reshape(-1, LN)

        tables, gram_items, late = gather_all(table.reshape(-1, LN), gram_part, 0, (as_rows(user_idx), as_rows(user_conf)))
        tables = tables.reshape(G, -1, F, LN)
        late = lax.all_to_all(late, 'g', 0, 0, tiled=True)
        user_t, user_table, gram_part = half_step(8, True, 2, 6, tables, payload.reshape(G * PAY, LN),
                                                  gram_items, start_block.T)
        user_tables, gram_users = gather_all(user_table.reshape(-1, LN), gram_part, 1)
        user_tables = user_tables.reshape(G, -1, F, LN)
        item_new = half_step(2, False, 2, 8, user_tables, late.reshape(G * PAY, LN), gram_users, item_t)[0]
        return user_t.T, item_new.T

    return jax.shard_map(local_sweep, mesh=mesh,
                         in_specs=(part_spec, part_spec, slot_spec, slot_spec, slot_spec, slot_spec),
                         out_specs=(part_spec, part_spec), check_vma=False)
```

```python
import functools

import jax
import jax.numpy as jnp
from jax import lax
from jax.experimental import pallas as pl
from jax.experimental.pallas import tpu as pltpu
from jax.sharding import PartitionSpec as P


REG_LAMBDA = 0.01
CG_STEPS = 3
F = 64
FX = F + 16
PITCH = F + 8
LN = 128
G = 128
PAY = 48
EMPTY = 2048
PACK = 4096
F32 = jnp.float32
BF16 = jnp.bfloat16
I16 = jnp.int16
I32 = jnp.int32


def iota(shape, dim, dtype=I32):
    return lax.broadcasted_iota(dtype, shape, dim)


def take(x, ind, axis):
    other = 1 - axis
    dims = lax.GatherDimensionNumbers(
        offset_dims=(), collapsed_slice_dims=(axis,), start_index_map=(axis,),
        operand_batching_dims=(other,), start_indices_batching_dims=(other,))
    return lax.gather(x, ind[..., None], dims, slice_sizes=(1, 1),
                      mode=lax.GatherScatterMode.PROMISE_IN_BOUNDS)


def dot_nt(a, b):
    return lax.dot_general(a, b, (((1,), (1,)), ((), ())), preferred_element_type=F32)


def fold(gram):
    return jnp.concatenate([gram[:F // 2], gram[F // 2:]], axis=1)


def unfold(gram):
    return jnp.concatenate([gram[:, :F], gram[:, F:]], axis=0)


def table_kernel(x_ref, tab_ref, gram_ref):
    x = x_ref[...].astype(BF16)
    for h in range(x.shape[1] // LN):
        tab_ref[h] = x[:, h * LN:(h + 1) * LN]
    gram_ref[...] = fold(dot_nt(x, x))


def make_table(x_t):
    n = x_t.shape[1]
    return pl.pallas_call(
        table_kernel,
        out_shape=(jax.ShapeDtypeStruct((n // LN, F, LN), BF16), jax.ShapeDtypeStruct((F // 2, LN), F32)),
        name='table',
    )(x_t)


def code_weight(idx, conf):
    code = jnp.where(conf > 0.0, idx, EMPTY).astype(F32)
    return code, jnp.maximum(conf - 1.0, 0.0)


def arrange_users(me, idx_ref, conf_ref, out_ref, send=None):
    skew = me % 16
    row, lane = iota((8, LN), 0), iota((8, LN), 1)
    first = (lane - 16 * row) & 127
    second = ((lane >> 4) - row) & 7
    third = ((lane ^ skew) + 16 * row) & 127
    dests = out_ref.shape[0]
    batch = min(8, dests)

    def arrange(x):
        return take(take(take(x, first, 1), second, 0), third, 1)

    def place(n, _):
        for e in range(batch):
            dest = (me + n * batch + e) % dests
            codes = []
            for q in range(4):
                cols = pl.ds(pl.multiple_of(dest * 512 + q * LN, LN), LN)
                code, weight = code_weight(idx_ref[:, cols], conf_ref[:, cols])
                out_ref[dest, pl.ds(q * 8, 8), :] = arrange(weight)
                codes.append(arrange(code))
            for q in range(2):
                out_ref[dest, pl.ds(32 + q * 8, 8), :] = codes[q] + PACK * codes[q + 2]

        if send is not None:
            @pl.when(n > 0)
            def _():
                for e in range(batch):
                    send((me + (n - 1) * batch + e) % dests)
        return 0

    lax.fori_loop(0, dests // batch, place, 0)

    def send_last():
        for e in range(batch):
            send((me + dests - batch + e) % dests)

    return send_last


def arrange_items(me, idx_ref, conf_ref, out_ref):
    skew = me % 64
    lane = iota((8, LN), 1)
    pattern = lane ^ skew
    low = lane < 64

    def halves(x0, x1):
        a = jnp.where(low, x0, pltpu.roll(x1, 64, 1))
        b = jnp.where(low, pltpu.roll(x0, 64, 1), x1)
        return take(a, pattern, 1), take(b, pattern, 1)

    def place(dest, _):
        for q in range(2):
            base = dest * 32 + q * 16
            rows = [pl.ds(base + j, 8, stride=2) for j in range(2)]
            pairs = [code_weight(idx_ref[r, :], conf_ref[r, :]) for r in rows]
            code_a, code_b = halves(pairs[0][0], pairs[1][0])
            weight_a, weight_b = halves(pairs[0][1], pairs[1][1])
            out_ref[dest, pl.ds(q * 8, 8), :] = weight_a
            out_ref[dest, pl.ds(16 + q * 8, 8), :] = weight_b
            out_ref[dest, pl.ds(32 + q * 8, 8), :] = code_a + PACK * code_b
        return 0

    lax.fori_loop(0, out_ref.shape[0], place, 0, unroll=min(8, out_ref.shape[0]))


ORDERS = ((2, 1, 0), (1, 0, 2), (0, 2, 1))
STRIDES = (32, 8, 2)
RING = 4


def gather_kernel(streams, beside_work, *refs):
    if beside_work:
        (table, gram, uidx_hbm, uconf_hbm, idx_hbm, conf_hbm, *outs, arrived, pay_hbm,
         send, recv, pass_send, pass_recv, local, uidx, uconf, upay, idx, conf, pay, work) = refs
        loads = [pltpu.make_async_copy(a, b, work.at[n]) for n, (a, b) in enumerate(
            ((uidx_hbm, uidx), (uconf_hbm, uconf), (idx_hbm, idx), (conf_hbm, conf)))]
        for copy in loads:
            copy.start()
    else:
        table, gram, *outs, send, recv, pass_send, pass_recv, local = refs
    ins = (table, gram)
    me = lax.axis_index('g')
    core = me % 2
    here = [me // stride % RING for stride in STRIDES]
    partner = me + 1 - 2 * core

    def beside(dim, delta):
        return me + ((here[dim] + delta + RING) % RING - here[dim]) * STRIDES[dim]

    barrier = pltpu.get_barrier_semaphore()
    if beside_work:
        def greet(n, _):
            pl.semaphore_signal(barrier, inc=1, device_id={'g': (me + n) % G}, device_id_type=pl.DeviceIdType.MESH)
            return 0

        lax.fori_loop(1, G, greet, 0)
        pl.semaphore_wait(barrier, G - 1)
    else:
        peers = [beside(dim, delta) for dim in range(3) for delta in (1, -1)] + [partner]
        for peer in peers:
            pl.semaphore_signal(barrier, inc=1, device_id={'g': peer}, device_id_type=pl.DeviceIdType.MESH)
        pl.semaphore_wait(barrier, len(peers))

    def region(s, phase, dim, delta, half):
        which, first, rows = streams[s][:3]
        order = ORDERS[streams[s][3]]
        index = []
        for d in range(3):
            if d in order[:phase]:
                index.append(pl.ds(0, RING))
            else:
                index.append((here[d] + delta + RING) % RING if d == dim else here[d])
        if half is not None:
            rows = rows // 2
            first = first + half * rows
        return outs[which].at[(*index, core, pl.ds(first, rows), slice(None))]

    def remote(src, dst, sems, index, peer):
        return pltpu.make_async_remote_copy(
            src_ref=src, dst_ref=dst, send_sem=sems[0].at[index], recv_sem=sems[1].at[index],
            device_id={'g': peer}, device_id_type=pl.DeviceIdType.MESH)

    passed = []

    def pass_on(src, dst, s, slot):
        copy = remote(src, dst, (pass_send, pass_recv), 13 * s + slot, partner)
        copy.start()
        passed.append(copy)

    count = len(streams)
    own, kept = [], []
    for s, (which, first, rows, _) in enumerate(streams):
        src = ins[which].at[pl.ds(first, rows), :]
        own.append(src)
        copy = pltpu.make_async_copy(src, region(s, 0, 0, 0, None), local.at[s])
        copy.start()
        kept.append(copy)
    sent, across, further = [], {}, {}

    def start_across(s, phase):
        dim = ORDERS[streams[s][3]][phase]
        for way, delta in enumerate((1, -1)):
            mine = region(s, phase, dim, 0, None)
            src = own[s] if phase == 0 else mine
            across[s, way] = remote(src, mine, (send, recv), ((s * 3 + phase) * 2 + 0) * 2 + way, beside(dim, delta))
            across[s, way].start()
            sent.append(across[s, way])

    def start_further(s, phase):
        dim = ORDERS[streams[s][3]][phase]
        for way, delta in enumerate((1, -1)):
            across[s, way].wait_recv()
            half = region(s, phase, dim, -delta, way)
            further[s, way] = remote(half, half, (send, recv), ((s * 3 + phase) * 2 + 1) * 2 + way, beside(dim, delta))
            further[s, way].start()
            sent.append(further[s, way])
        for way, delta in enumerate((1, -1)):
            whole = region(s, phase, dim, -delta, None)
            pass_on(whole, whole, s, 1 + 4 * phase + way)

    def finish(s, phase):
        dim = ORDERS[streams[s][3]][phase]
        for way in range(2):
            further[s, way].wait_recv()
        if phase == 0:
            kept[s].wait()
        if phase < 2:
            start_across(s, phase + 1)
        for way in range(2):
            half = region(s, phase, dim, 2, way)
            pass_on(half, half, s, 3 + 4 * phase + way)

    for s in range(count):
        start_across(s, 0)
    for s in range(count):
        pass_on(own[s], region(s, 0, 0, 0, None), s, 0)
    if beside_work:
        def send_user(dest):
            @pl.when(dest != me)
            def _():
                pltpu.make_async_remote_copy(
                    src_ref=upay.at[dest], dst_ref=arrived.at[me], send_sem=work.at[4], recv_sem=work.at[5],
                    device_id={'g': dest}, device_id_type=pl.DeviceIdType.MESH).start()

        loads[0].wait()
        loads[1].wait()
        send_last = arrange_users(me, uidx, uconf, upay, send_user)
    for phase in range(3):
        for s in range(count):
            start_further(s, phase)
        if phase == 0 and beside_work:
            send_last()
            stay = pltpu.make_async_copy(upay.at[me], arrived.at[me], work.at[7])
            stay.start()
        if phase == 2 and beside_work:
            store = pltpu.make_async_copy(pay, pay_hbm, work.at[6])
            store.start()
        for s in range(count):
            finish(s, phase)
        if phase == 1 and beside_work:
            loads[2].wait()
            loads[3].wait()
            arrange_items(me, idx, conf, pay)
    if beside_work:
        store.wait()
        stay.wait()
        others = pl.ds(0, G - 1)
        pltpu.make_async_copy(upay.at[others], upay.at[others], work.at[4]).wait()
        pltpu.make_async_copy(arrived.at[others], arrived.at[others], work.at[5]).wait()
    for copy in sent:
        copy.wait_send()
    for copy in passed:
        copy.wait_send()
    for copy in passed:
        copy.wait_recv()


def gather_all(table, gram, collective_id, user_slots=(), item_slots=()):
    rows = table.shape[0]
    units = rows // 16
    large = -(-units // 6)
    sizes = (large, large, (units - 4 * large) // 2) * 2
    streams, first = [(1, 0, gram.shape[0], 2)], 0
    for n, size in enumerate(sizes):
        streams.append((0, first, 16 * size, n % 3))
        first += 16 * size
    count = len(streams)
    any_spec = pl.BlockSpec(memory_space=pl.ANY)
    out_shape = [jax.ShapeDtypeStruct((RING, RING, RING, 2, *x.shape), x.dtype) for x in (table, gram)]
    scratch = [pltpu.SemaphoreType.DMA((12 * count,)), pltpu.SemaphoreType.DMA((12 * count,)),
               pltpu.SemaphoreType.DMA((13 * count,)), pltpu.SemaphoreType.DMA((13 * count,)),
               pltpu.SemaphoreType.DMA((count,))]
    slots = (*user_slots, *item_slots)
    if slots:
        out_shape += [jax.ShapeDtypeStruct((G, PAY, LN), F32)] * 2
        for pair in (user_slots, item_slots):
            scratch += [pltpu.VMEM(x.shape, x.dtype) for x in pair] + [pltpu.VMEM((G, PAY, LN), F32)]
        scratch.append(pltpu.SemaphoreType.DMA((8,)))
    tables, grams, *payload = pl.pallas_call(
        functools.partial(gather_kernel, tuple(streams), bool(slots)),
        in_specs=[pl.BlockSpec(memory_space=pltpu.VMEM)] * 2 + [any_spec] * len(slots),
        out_specs=[any_spec] * len(out_shape),
        out_shape=out_shape,
        scratch_shapes=scratch,
        compiler_params=pltpu.CompilerParams(collective_id=collective_id, has_side_effects=True),
        name='gather_all',
    )(table, gram, *slots)
    return tables.reshape(G, rows, LN), grams.reshape(-1, LN), *payload


def half_kernel(slots, blocks, pair, lanes_of, body, emit, tab_hbm, pay_hbm, gram_ref, x0_ref, *refs):
    if emit:
        out_ref, tab_ref, gout_ref = refs[:3]
        refs = refs[3:]
    else:
        out_ref = refs[0]
        refs = refs[1:]
    tab, pay, ids, yu_a, yu_b, wu_a, wu_b, a_scr, at_scr, p_scr, s_scr, sems = refs
    per = LN // slots
    chunks = G // per
    groups = LN // per
    steps = blocks * groups // pair
    turns = groups // pair
    heads = tab.shape[1]

    pay_copy = pltpu.make_async_copy(pay_hbm, pay, sems.at[8])
    pay_copy.start()

    def tab_copy(i):
        return pltpu.make_async_copy(tab_hbm.at[pl.ds(16 * i, 16)], tab.at[pl.ds(16 * i, 16)], sems.at[i])

    for i in range(8):
        tab_copy(i).start()
    ids[...] = iota((2 * LN, LN), 0, I16)
    pay_copy.wait()

    lane16 = iota((16, LN), 1, I16)
    lane = iota((8, LN), 1)
    row = iota((8, LN), 0)

    def add_gram(d, acc):
        return acc + gram_ref[pl.ds(pl.multiple_of(d * (F // 2), F // 2), F // 2), :]

    gram = lax.fori_loop(0, G, add_gram, jnp.zeros((F // 2, LN), F32), unroll=8)
    gpad = jnp.concatenate([unfold(gram), jnp.zeros((16, F), F32)], axis=0)
    gpad = jnp.concatenate([gpad, jnp.zeros((FX, 16), F32)], axis=1)
    rr, cc = iota((FX, FX), 0), iota((FX, FX), 1)
    gpad = gpad + jnp.where((rr == cc) & (rr < F), REG_LAMBDA, 0.0)

    def pay_row(t):
        if slots == 8:
            return t, 32 + t % 16, 12 * (t // 16)
        return (t % 2) * 16 + t // 2, 32 + t // 2, 12 * (t % 2)

    def spread_weights(t, wu, q):
        wrow = pay_row(t)[0]
        for c in range(chunks):
            tiles = []
            for v in range(per // 8):
                start = (per * c + 8 * v) * PAY + wrow
                tiles.append(pay[pl.ds(start, 8, stride=PAY), :])
            for bit in (1, 2, 4):
                hit = (lane & bit) != 0
                up = (row & bit) != 0
                for v in range(len(tiles)):
                    x = tiles[v]
                    if bit == 4:
                        other = pltpu.roll(x, 4, 0)
                    else:
                        other = jnp.where(up, pltpu.roll(x, bit, 0), pltpu.roll(x, 8 - bit, 0))
                    tiles[v] = jnp.where(hit, other, x)
            bit = 8
            while bit < per:
                hit = (lane & bit) != 0
                tiles = [jnp.where(hit, tiles[v ^ (bit // 8)], tiles[v]) for v in range(len(tiles))]
                bit *= 2
            for v in range(len(tiles)):
                wu[c, pl.ds(per * q + 8 * v, 8), :] = tiles[v]

    def exchange(xs, low_bit):
        bit, n = 1, len(xs)
        while bit < n:
            hit = (lane16 & I16(bit * low_bit)) != I16(0)
            xs = [jnp.where(hit, xs[a ^ bit], xs[a]) for a in range(n)]
            bit *= 2
        return xs

    ones = jnp.ones((16, LN * chunks), BF16)

    def form(y_parts, wu, u, at):
        vs = []
        for c in range(chunks):
            w = wu[c, pl.ds(u, 1), :]
            vs.append((y_parts[c].astype(F32) * w).astype(BF16))
        y = jnp.concatenate([jnp.concatenate(y_parts, axis=1), ones], axis=0)
        v = jnp.concatenate([jnp.concatenate(vs, axis=1), ones], axis=0)
        a_scr[pl.ds(at * PITCH, PITCH), pl.ds(0, FX)] = (dot_nt(y, v) + gpad)[:PITCH]

    def form_rows(t, i, yu, wu):
        first = (t - 1) // turns % 2 * LN + (t - 1) % turns * (per * pair)
        rows = [per * (i // 4) + i % 4 + 4 * m for m in range(per // 4)]
        parts = []
        for c in range(chunks):
            by_k = [exchange([yu[u, c, pl.ds(16 * k, 16), :] for u in rows], 4) for k in range(4)]
            parts.append([jnp.concatenate([x[m] for x in by_k], axis=0) for m in range(len(rows))])
        for m, u in enumerate(rows):
            form([parts[c][m] for c in range(chunks)], wu, u, first + u)

    def codes(t, d, q):
        _, crow, shift = pay_row(pair * t + q)
        packed = pay[pl.ds(d * PAY + crow, 1), :].astype(I32)
        return (packed >> shift) & (PACK - 1)

    def by_lanes(t, d, q):
        code = jnp.broadcast_to(codes(t, d, q), (F, LN)).astype(I16)
        low = code & I16(LN - 1)
        head = code >> I16(7)
        acc = jnp.zeros((F, LN), BF16)
        for h in range(heads):
            acc = jnp.where(head == I16(h), take(tab[d, h], low, 1), acc)
        return acc

    def by_matmul(t, d):
        hots, halves = [], []
        for q in range(2):
            code = codes(t, d, q)
            low = (jnp.broadcast_to(code, (2 * LN, LN)) & (2 * LN - 1)).astype(I16)
            hots.append(jnp.where(low == ids[...], jnp.ones((2 * LN, LN), BF16), jnp.zeros((2 * LN, LN), BF16)))
            halves.append(jnp.broadcast_to(code, (F, LN)) >> 8)
        table = jnp.concatenate([jnp.concatenate([tab[d, 2 * h], tab[d, 2 * h + 1]], axis=1)
                                 for h in range(heads // 2)], axis=0)
        found = jnp.dot(table, jnp.concatenate(hots, axis=1), preferred_element_type=F32)
        out = []
        for q in range(2):
            acc = jnp.zeros((F, LN), F32)
            for h in range(heads // 2):
                acc = jnp.where(halves[q] == h, found[h * F:(h + 1) * F, q * LN:(q + 1) * LN], acc)
            out.append(acc.astype(BF16))
        return out

    def lookup(t, i, yu):
        turn = 0
        for quad in range(4):
            found = []
            for dd in range(4):
                d = 16 * i + 4 * quad + dd
                turn += lanes_of
                if turn >= 16:
                    turn -= 16
                    found.append([by_lanes(t, d, q) for q in range(pair)])
                else:
                    found.append(by_matmul(t, d))
            for q in range(pair):
                for k in range(4):
                    rows = slice(16 * k, 16 * k + 16)
                    xs = exchange([x[q][rows] for x in found], 1)
                    for a in range(4):
                        if slots == 8:
                            yu[16 * q + 4 * quad + a, i, rows, :] = xs[a]
                        else:
                            yu[64 * q + (i % 4) * 16 + 4 * quad + a, i // 4, rows, :] = xs[a]

    def flip(block, b):
        m = a_scr[pl.ds(block % 2 * (LN * PITCH) + b, LN, stride=PITCH), :].T
        at_scr[b] = m[:F]
        s_scr[pl.ds(b, 1), :] = m[F:F + 1]

    def flip_all(block):
        def four(b4, _):
            for e in range(4):
                flip(block, 4 * b4 + e)
            return 0

        lax.fori_loop(0, F // 4, four, 0)

    def solve(block):
        rhs = a_scr[pl.ds(block % 2 * (LN * PITCH) + F, LN, stride=PITCH), :].T[:F] + s_scr[...]
        x = x0_ref[:, pl.ds(pl.multiple_of(block * LN, LN), LN)]

        def apply_mat(vec):
            p_scr[...] = vec

            def add(b, acc):
                return acc + at_scr[b] * p_scr[pl.ds(b, 1), :]

            return lax.fori_loop(0, F, add, jnp.zeros((F, LN), F32), unroll=8)

        res = rhs - apply_mat(x)
        direction = res
        res_sq = jnp.sum(res * res, axis=0, keepdims=True)
        for step in range(CG_STEPS):
            q = apply_mat(direction)
            length = res_sq / jnp.sum(direction * q, axis=0, keepdims=True)
            x = x + length * direction
            if step + 1 < CG_STEPS:
                res = res - length * q
                new_sq = jnp.sum(res * res, axis=0, keepdims=True)
                direction = res + (new_sq / res_sq) * direction
                res_sq = new_sq
        out_ref[:, pl.ds(pl.multiple_of(block * LN, LN), LN)] = x
        if emit:
            xb = x.astype(BF16)
            tab_ref[block] = xb
            gout_ref[...] += fold(dot_nt(xb, xb))

    if emit:
        gout_ref[...] = jnp.zeros((F // 2, LN), F32)

    def weights(t, wu):
        for q in range(pair):
            spread_weights(pair * t + q, wu, q)

    def first_pass():
        weights(0, wu_a)

        def inner(i, _):
            tab_copy(i).wait()
            lookup(0, i, yu_a)
            return 0

        lax.fori_loop(0, 8, inner, 0)

    def step_pass(t, ahead, count, size, yu, wu, yu_last, wu_last):
        before = jnp.maximum((t - 1) // turns - 1, 0)
        if ahead:
            weights(jnp.minimum(t, steps - 1), wu)

        def inner(i2, _):
            flips = F // (8 * turns)
            for i in range(size):
                i = size * i2 + i
                for e in range(flips):
                    flip(before, ((t - 1) % turns * 8 + i) * flips + e)
                form_rows(t, i, yu_last, wu_last)
                if ahead:
                    lookup(t, i, yu)
            return 0

        lax.fori_loop(0, count, inner, 0)

        def finish_block():
            @pl.when((t >= turns + 1) & (t % turns == 0))
            def _():
                solve(t // turns - 2)

        if ahead:
            pl.when(t < steps)(finish_block)
        else:
            finish_block()

    def two_steps(j, _):
        step_pass(2 * j + 1, True, 8 // body, body, yu_b, wu_b, yu_a, wu_a)
        step_pass(2 * j + 2, True, jnp.where(2 * j + 2 < steps, 8 // body, 0), body, yu_a, wu_a, yu_b, wu_b)
        return 0

    first_pass()
    lax.fori_loop(0, steps // 2, two_steps, 0)
    step_pass(steps, False, 8, 1, None, None, yu_b, wu_b)
    flip_all(blocks - 1)
    solve(blocks - 1)


def half_step(slots, emit, pair, lanes_of, body, tables, payload, gram, x0_t):
    n = x0_t.shape[1]
    heads = tables.shape[1]
    per = LN // slots
    chunks = G // per
    out_shape = [jax.ShapeDtypeStruct((F, n), F32)]
    if emit:
        out_shape += [jax.ShapeDtypeStruct((n // LN, F, LN), BF16), jax.ShapeDtypeStruct((F // 2, LN), F32)]
    vmem = pl.BlockSpec(memory_space=pltpu.VMEM)
    return pl.pallas_call(
        functools.partial(half_kernel, slots, n // LN, pair, lanes_of, body, emit),
        in_specs=[pl.BlockSpec(memory_space=pl.ANY), pl.BlockSpec(memory_space=pl.ANY), vmem, vmem],
        out_specs=[vmem] * len(out_shape),
        out_shape=out_shape,
        scratch_shapes=[
            pltpu.VMEM((G, heads, F, LN), BF16),
            pltpu.VMEM((G * PAY, LN), F32),
            pltpu.VMEM((2 * LN, LN), I16),
            pltpu.VMEM((pair * per, chunks, F, LN), BF16),
            pltpu.VMEM((pair * per, chunks, F, LN), BF16),
            pltpu.VMEM((chunks, pair * per, LN), F32),
            pltpu.VMEM((chunks, pair * per, LN), F32),
            pltpu.VMEM((2 * LN * PITCH, LN), F32),
            pltpu.VMEM((F, F, LN), F32),
            pltpu.VMEM((F, LN), F32),
            pltpu.VMEM((F, LN), F32),
            pltpu.SemaphoreType.DMA((9,)),
        ],
        compiler_params=pltpu.CompilerParams(vmem_limit_bytes=62 * 1024 * 1024),
        cost_estimate=pl.CostEstimate(flops=10 ** 11, bytes_accessed=2 ** 25, transcendentals=0),
        name='half_step',
    )(tables, payload, gram, x0_t)


def solution(mesh):
    part_spec = P(('tables', 'g'), None)
    slot_spec = P(('tables', 'g'), None, None)

    def local_sweep(item_block, start_block, item_idx, item_conf, user_idx, user_conf):
        item_t = item_block.T
        table, gram_part = make_table(item_t)

        def as_rows(x):
            return x[0].reshape(-1, LN, 2).transpose(0, 2, 1).reshape(-1, LN)

        tables, gram_items, payload, late = gather_all(
            table.reshape(-1, LN), gram_part, 0, (item_idx[0].T, item_conf[0].T), (as_rows(user_idx), as_rows(user_conf)))
        tables = tables.reshape(G, -1, F, LN)
        late = lax.all_to_all(late, 'g', 0, 0, tiled=True)
        user_t, user_table, gram_part = half_step(8, True, 2, 6, 2, tables, payload.reshape(G * PAY, LN),
                                                  gram_items, start_block.T)
        user_tables, gram_users = gather_all(user_table.reshape(-1, LN), gram_part, 1)
        user_tables = user_tables.reshape(G, -1, F, LN)
        item_new = half_step(2, False, 2, 7, 1, user_tables, late.reshape(G * PAY, LN), gram_users, item_t)[0]
        return user_t.T, item_new.T

    return jax.shard_map(local_sweep, mesh=mesh,
                         in_specs=(part_spec, part_spec, slot_spec, slot_spec, slot_spec, slot_spec),
                         out_specs=(part_spec, part_spec), check_vma=False)
```

```python
import functools

import jax
import jax.numpy as jnp
from jax import lax
from jax.experimental import pallas as pl
from jax.experimental.pallas import tpu as pltpu
from jax.sharding import PartitionSpec as P


REG_LAMBDA = 0.01
CG_STEPS = 3
F = 64
FX = F + 16
PITCH = F + 8
LN = 128
G = 128
PAY = 48
EMPTY = 2048
PACK = 4096
F32 = jnp.float32
BF16 = jnp.bfloat16
I16 = jnp.int16
I32 = jnp.int32


def iota(shape, dim, dtype=I32):
    return lax.broadcasted_iota(dtype, shape, dim)


def take(x, ind, axis):
    other = 1 - axis
    dims = lax.GatherDimensionNumbers(
        offset_dims=(), collapsed_slice_dims=(axis,), start_index_map=(axis,),
        operand_batching_dims=(other,), start_indices_batching_dims=(other,))
    return lax.gather(x, ind[..., None], dims, slice_sizes=(1, 1),
                      mode=lax.GatherScatterMode.PROMISE_IN_BOUNDS)


def dot_nt(a, b):
    return lax.dot_general(a, b, (((1,), (1,)), ((), ())), preferred_element_type=F32)


def fold(gram):
    return jnp.concatenate([gram[:F // 2], gram[F // 2:]], axis=1)


def unfold(gram):
    return jnp.concatenate([gram[:, :F], gram[:, F:]], axis=0)


def make_table(x_ref, tab_ref, gram_ref):
    x = x_ref[...].astype(BF16)
    for h in range(x.shape[1] // LN):
        tab_ref[h * F:(h + 1) * F, :] = x[:, h * LN:(h + 1) * LN]
    gram_ref[...] = fold(dot_nt(x, x))


def code_weight(idx, conf):
    code = jnp.where(conf > 0.0, idx, EMPTY).astype(F32)
    return code, jnp.maximum(conf - 1.0, 0.0)


def arrange_users(me, idx_ref, conf_ref, out_ref, begin=0, end=None):
    skew = me % 16
    row, lane = iota((8, LN), 0), iota((8, LN), 1)
    first = (lane - 16 * row) & 127
    second = ((lane >> 4) - row) & 7
    third = ((lane ^ skew) + 16 * row) & 127
    dests = idx_ref.shape[1] // 512
    batch = min(8, dests)

    def arrange(x):
        return take(take(take(x, first, 1), second, 0), third, 1)

    def place(n, _):
        for e in range(batch):
            dest = n * batch + e
            owner = (dest // 32, dest // 8 % 4, dest // 2 % 4, dest % 2)
            codes = []
            for q in range(4):
                cols = pl.ds(pl.multiple_of(dest * 512 + q * LN, LN), LN)
                code, weight = code_weight(idx_ref[:, cols], conf_ref[:, cols])
                out_ref[(*owner, pl.ds(q * 8, 8), slice(None))] = arrange(weight)
                codes.append(arrange(code))
            for q in range(2):
                out_ref[(*owner, pl.ds(32 + q * 8, 8), slice(None))] = codes[q] + PACK * codes[q + 2]
        return 0

    lax.fori_loop(begin, dests // batch if end is None else end, place, 0)


def arrange_items(me, idx_ref, conf_ref, out_ref):
    skew = me % 64
    lane = iota((8, LN), 1)
    pattern = lane ^ skew
    low = lane < 64

    def halves(x0, x1):
        a = jnp.where(low, x0, pltpu.roll(x1, 64, 1))
        b = jnp.where(low, pltpu.roll(x0, 64, 1), x1)
        return take(a, pattern, 1), take(b, pattern, 1)

    def place(dest, _):
        for q in range(2):
            base = dest * 32 + q * 16
            rows = [pl.ds(base + j, 8, stride=2) for j in range(2)]
            pairs = [code_weight(idx_ref[r, :], conf_ref[r, :]) for r in rows]
            code_a, code_b = halves(pairs[0][0], pairs[1][0])
            weight_a, weight_b = halves(pairs[0][1], pairs[1][1])
            out_ref[dest, pl.ds(q * 8, 8), :] = weight_a
            out_ref[dest, pl.ds(16 + q * 8, 8), :] = weight_b
            out_ref[dest, pl.ds(32 + q * 8, 8), :] = code_a + PACK * code_b
        return 0

    lax.fori_loop(0, out_ref.shape[0], place, 0, unroll=min(8, out_ref.shape[0]))


ORDERS = ((2, 1, 0), (1, 0, 2), (0, 2, 1))
STRIDES = (32, 8, 2)
RING = 4


def gather_kernel(streams, beside_work, *refs):
    if beside_work:
        (rows_ref, uidx_hbm, uconf_hbm, idx_hbm, conf_hbm, *outs, arrived, pay_hbm,
         send, recv, pass_send, pass_recv, local, uidx, uconf, idx, conf, pay, stage, relay,
         swap_send, swap_recv, work, table, gram) = refs
        loads = [pltpu.make_async_copy(a, b, work.at[n]) for n, (a, b) in enumerate(
            ((uidx_hbm, uidx), (uconf_hbm, uconf), (idx_hbm, idx), (conf_hbm, conf)))]
        for copy in loads:
            copy.start()
        make_table(rows_ref, table, gram)
    else:
        table, gram, *outs, send, recv, pass_send, pass_recv, local, table_land, gram_land = refs
    ins = (table, gram)
    lands = outs if beside_work else (table_land, gram_land)
    me = lax.axis_index('g')
    core = me % 2
    here = [me // stride % RING for stride in STRIDES]
    partner = me + 1 - 2 * core

    def beside(dim, delta):
        return me + ((here[dim] + delta + RING) % RING - here[dim]) * STRIDES[dim]

    barrier = pltpu.get_barrier_semaphore()
    peers = [beside(dim, delta) for dim in range(3) for delta in (1, -1)] + [partner]
    for peer in peers:
        pl.semaphore_signal(barrier, inc=1, device_id={'g': peer}, device_id_type=pl.DeviceIdType.MESH)
    pl.semaphore_wait(barrier, len(peers))

    def region(s, phase, dim, delta, half):
        which, first, rows = streams[s][:3]
        order = ORDERS[streams[s][3]]
        index = []
        for d in range(3):
            if d in order[:phase]:
                index.append(pl.ds(0, RING))
            else:
                index.append((here[d] + delta + RING) % RING if d == dim else here[d])
        if half is not None:
            rows = rows // 2
            first = first + half * rows
        return lands[which].at[(*index, core, pl.ds(first, rows), slice(None))]

    def remote(src, dst, sems, index, peer):
        return pltpu.make_async_remote_copy(
            src_ref=src, dst_ref=dst, send_sem=sems[0].at[index], recv_sem=sems[1].at[index],
            device_id={'g': peer}, device_id_type=pl.DeviceIdType.MESH)

    swaps = {}

    def slab(level, dim, delta, color, half=None):
        index = [pl.ds(0, RING)] * 3
        index[dim] = (here[dim] + delta + RING) % RING
        rows = pl.ds(16 * color, 16) if half is None else pl.ds(16 * color + 8 * half, 8)
        return stage.at[(level, *index, pl.ds(0, 2), rows, slice(None))]

    def swap(src, dst, index, peer):
        copy = remote(src, dst, (swap_send, swap_recv), index, peer)
        copy.start()
        swaps[index] = copy

    def swap_start(phase):
        for color in range(3):
            dim = ORDERS[color][phase]
            base = (phase * 3 + color) * 6
            for way, delta in enumerate((1, -1)):
                swap(slab(phase, dim, delta, color), slab(phase + 1, dim, 0, color), base + way, beside(dim, delta))
                swap(slab(phase, dim, 2, color, way), relay.at[phase, color, way], base + 2 + way, beside(dim, delta))
        for color in range(3):
            dim = ORDERS[color][phase]
            index = [pl.ds(0, RING)] * 3
            index[dim] = pl.ds(here[dim], 1)
            part = (*index, pl.ds(0, 2), pl.ds(16 * color, 16), slice(None))
            stage[(phase + 1, *part)] = stage[(phase, *part)]

    def swap_further(phase):
        for color in range(3):
            dim = ORDERS[color][phase]
            base = (phase * 3 + color) * 6
            for way, delta in enumerate((1, -1)):
                swaps[base + 2 + way].wait_recv()
                swap(relay.at[phase, color, way], slab(phase + 1, dim, -delta, color, way), base + 4 + way, beside(dim, delta))

    def swap_finish(phase):
        for color in range(3):
            base = (phase * 3 + color) * 6
            for n in (0, 1, 4, 5):
                swaps[base + n].wait_recv()

    def swap_cores():
        everywhere = [pl.ds(0, RING)] * 3
        mine = arrived.at[(*everywhere, core)]
        swap(stage.at[(3, *everywhere, 1 - core)], mine, 54, partner)
        stay = pltpu.make_async_copy(stage.at[(3, *everywhere, core)], mine, work.at[4])
        stay.start()
        stay.wait()
        for copy in swaps.values():
            copy.wait_send()
        swaps[54].wait_recv()

    passed = {s: [] for s in range(len(streams))}

    def pass_on(src, dst, s, slot):
        copy = remote(src, dst, (pass_send, pass_recv), 13 * s + slot, partner)
        copy.start()
        passed[s].append(copy)

    count = len(streams)
    own, kept = [], []
    for s, (which, first, rows, _) in enumerate(streams):
        src = ins[which].at[pl.ds(first, rows), :]
        own.append(src)
        if beside_work:
            copy = pltpu.make_async_copy(src, region(s, 0, 0, 0, None), local.at[s])
            copy.start()
            kept.append(copy)
    if not beside_work:
        for land, mine in zip(lands, ins):
            land[(*here, core)] = mine[...]
    sent, across, further = [], {}, {}

    def start_across(s, phase):
        dim = ORDERS[streams[s][3]][phase]
        for way, delta in enumerate((1, -1)):
            mine = region(s, phase, dim, 0, None)
            src = own[s] if phase == 0 else mine
            across[s, way] = remote(src, mine, (send, recv), ((s * 3 + phase) * 2 + 0) * 2 + way, beside(dim, delta))
            across[s, way].start()
            sent.append(across[s, way])

    def start_further(s, phase):
        dim = ORDERS[streams[s][3]][phase]
        for way, delta in enumerate((1, -1)):
            across[s, way].wait_recv()
            half = region(s, phase, dim, -delta, way)
            further[s, way] = remote(half, half, (send, recv), ((s * 3 + phase) * 2 + 1) * 2 + way, beside(dim, delta))
            further[s, way].start()
            sent.append(further[s, way])
        for way, delta in enumerate((1, -1)):
            whole = region(s, phase, dim, -delta, None)
            pass_on(whole, whole, s, 1 + 4 * phase + way)

    def finish(s, phase):
        dim = ORDERS[streams[s][3]][phase]
        for way in range(2):
            further[s, way].wait_recv()
        if phase == 0 and beside_work:
            kept[s].wait()
        if phase < 2:
            start_across(s, phase + 1)
        for way in range(2):
            half = region(s, phase, dim, 2, way)
            pass_on(half, half, s, 3 + 4 * phase + way)

    for s in range(count):
        start_across(s, 0)
    for s in range(count):
        pass_on(own[s], region(s, 0, 0, 0, None), s, 0)

    def every(step, phase):
        for s in range(count):
            step(s, phase)

    if beside_work:
        loads[0].wait()
        loads[1].wait()
        arrange_users(me, uidx, uconf, stage.at[0], 0, 8)
        every(start_further, 0)
        arrange_users(me, uidx, uconf, stage.at[0], 8, 16)
        every(finish, 0)
        swap_start(0)
        swap_further(0)
        every(start_further, 1)
        swap_finish(0)
        swap_start(1)
        loads[2].wait()
        loads[3].wait()
        arrange_items(me, idx, conf, pay)
        swap_further(1)
        swap_finish(1)
        swap_start(2)
        every(finish, 1)
        store = pltpu.make_async_copy(pay, pay_hbm, work.at[5])
        store.start()
        swap_further(2)
        every(start_further, 2)
        every(finish, 2)
        swap_finish(2)
        swap_cores()
        store.wait()
    else:
        for phase in range(3):
            every(start_further, phase)
            every(finish, phase)
    stores = []

    def put_out(s, which_core):
        which, first, rows, _ = streams[s]
        part = (*[pl.ds(0, RING)] * 3, which_core, pl.ds(first, rows), slice(None))
        copy = pltpu.make_async_copy(lands[which].at[part], outs[which].at[part], local.at[2 * s + len(stores) // count])
        copy.start()
        stores.append(copy)

    if not beside_work:
        for s in range(count):
            put_out(s, core)
    for s in range(count):
        for copy in passed[s]:
            copy.wait_recv()
        if not beside_work:
            put_out(s, 1 - core)
    for copy in sent:
        copy.wait_send()
    for s in range(count):
        for copy in passed[s]:
            copy.wait_send()
    for copy in stores:
        copy.wait()


def gather_all(sources, shapes, collective_id, slots=()):
    table, gram = shapes
    rows = table.shape[0]
    units = rows // 16
    large = -(-units // 6)
    sizes = (large, large, (units - 4 * large) // 2) * 2
    streams, first = [(1, 0, gram.shape[0], 2)], 0
    for n, size in enumerate(sizes):
        streams.append((0, first, 16 * size, n % 3))
        first += 16 * size
    count = len(streams)
    any_spec = pl.BlockSpec(memory_space=pl.ANY)
    out_shape = [jax.ShapeDtypeStruct((RING, RING, RING, 2, *x.shape), x.dtype) for x in shapes]
    scratch = [pltpu.SemaphoreType.DMA((12 * count,)), pltpu.SemaphoreType.DMA((12 * count,)),
               pltpu.SemaphoreType.DMA((13 * count,)), pltpu.SemaphoreType.DMA((13 * count,)),
               pltpu.SemaphoreType.DMA((2 * count,))]
    if slots:
        blocks = (RING, RING, RING, 2, PAY, LN)
        out_shape += [jax.ShapeDtypeStruct(blocks, F32), jax.ShapeDtypeStruct((G, PAY, LN), F32)]
        scratch += [pltpu.VMEM(x.shape, x.dtype) for x in slots]
        scratch += [pltpu.VMEM((G, PAY, LN), F32), pltpu.VMEM((4, *blocks), F32),
                    pltpu.VMEM((3, 3, 2, RING, RING, 2, 8, LN), F32),
                    pltpu.SemaphoreType.DMA((55,)), pltpu.SemaphoreType.DMA((55,)), pltpu.SemaphoreType.DMA((6,)),
                    pltpu.VMEM(table.shape, table.dtype), pltpu.VMEM(gram.shape, gram.dtype)]
    else:
        scratch += [pltpu.VMEM(x.shape, x.dtype) for x in out_shape]
    tables, grams, *payload = pl.pallas_call(
        functools.partial(gather_kernel, tuple(streams), bool(slots)),
        in_specs=[pl.BlockSpec(memory_space=pltpu.VMEM)] * len(sources) + [any_spec] * len(slots),
        out_specs=[any_spec] * len(out_shape),
        out_shape=out_shape,
        scratch_shapes=scratch,
        compiler_params=pltpu.CompilerParams(collective_id=collective_id, has_side_effects=True),
        name='gather_all',
    )(*sources, *slots)
    return tables.reshape(G, -1, F, LN), grams.reshape(-1, LN), *payload


def half_kernel(slots, blocks, pair, lanes_of, body, emit, tab_hbm, pay_hbm, gram_ref, x0_ref, *refs):
    if emit:
        out_ref, tab_ref, gout_ref = refs[:3]
        refs = refs[3:]
    else:
        out_ref = refs[0]
        refs = refs[1:]
    tab, pay, ids, yu_a, yu_b, wu_a, wu_b, a_scr, at_scr, p_scr, s_scr, sems = refs
    per = LN // slots
    chunks = G // per
    groups = LN // per
    steps = blocks * groups // pair
    turns = groups // pair
    heads = tab.shape[1]

    pay_copy = pltpu.make_async_copy(pay_hbm, pay, sems.at[8])
    pay_copy.start()

    def tab_copy(i):
        return pltpu.make_async_copy(tab_hbm.at[pl.ds(16 * i, 16)], tab.at[pl.ds(16 * i, 16)], sems.at[i])

    for i in range(8):
        tab_copy(i).start()
    ids[...] = iota((2 * LN, LN), 0, I16)
    pay_copy.wait()

    lane16 = iota((16, LN), 1, I16)
    lane = iota((8, LN), 1)
    row = iota((8, LN), 0)

    def add_gram(d, acc):
        return acc + gram_ref[pl.ds(pl.multiple_of(d * (F // 2), F // 2), F // 2), :]

    gram = lax.fori_loop(0, G, add_gram, jnp.zeros((F // 2, LN), F32), unroll=8)
    gpad = jnp.concatenate([unfold(gram), jnp.zeros((16, F), F32)], axis=0)
    gpad = jnp.concatenate([gpad, jnp.zeros((FX, 16), F32)], axis=1)
    rr, cc = iota((FX, FX), 0), iota((FX, FX), 1)
    gpad = gpad + jnp.where((rr == cc) & (rr < F), REG_LAMBDA, 0.0)

    def pay_row(t):
        if slots == 8:
            return t, 32 + t % 16, 12 * (t // 16)
        return (t % 2) * 16 + t // 2, 32 + t // 2, 12 * (t % 2)

    def spread_weights(t, wu, q):
        wrow = pay_row(t)[0]
        for c in range(chunks):
            tiles = []
            for v in range(per // 8):
                start = (per * c + 8 * v) * PAY + wrow
                tiles.append(pay[pl.ds(start, 8, stride=PAY), :])
            for bit in (1, 2, 4):
                hit = (lane & bit) != 0
                up = (row & bit) != 0
                for v in range(len(tiles)):
                    x = tiles[v]
                    if bit == 4:
                        other = pltpu.roll(x, 4, 0)
                    else:
                        other = jnp.where(up, pltpu.roll(x, bit, 0), pltpu.roll(x, 8 - bit, 0))
                    tiles[v] = jnp.where(hit, other, x)
            bit = 8
            while bit < per:
                hit = (lane & bit) != 0
                tiles = [jnp.where(hit, tiles[v ^ (bit // 8)], tiles[v]) for v in range(len(tiles))]
                bit *= 2
            for v in range(len(tiles)):
                wu[c, pl.ds(per * q + 8 * v, 8), :] = tiles[v]

    def exchange(xs, low_bit):
        bit, n = 1, len(xs)
        while bit < n:
            hit = (lane16 & I16(bit * low_bit)) != I16(0)
            xs = [jnp.where(hit, xs[a ^ bit], xs[a]) for a in range(n)]
            bit *= 2
        return xs

    ones = jnp.ones((16, LN * chunks), BF16)

    def form(y_parts, wu, u, at):
        vs = []
        for c in range(chunks):
            w = wu[c, pl.ds(u, 1), :]
            vs.append((y_parts[c].astype(F32) * w).astype(BF16))
        y = jnp.concatenate([jnp.concatenate(y_parts, axis=1), ones], axis=0)
        v = jnp.concatenate([jnp.concatenate(vs, axis=1), ones], axis=0)
        a_scr[pl.ds(at * PITCH, PITCH), pl.ds(0, FX)] = (dot_nt(y, v) + gpad)[:PITCH]

    def form_rows(t, i, yu, wu):
        first = (t - 1) // turns % 2 * LN + (t - 1) % turns * (per * pair)
        rows = [per * (i // 4) + i % 4 + 4 * m for m in range(per // 4)]
        parts = []
        for c in range(chunks):
            by_k = [exchange([yu[u, c, pl.ds(16 * k, 16), :] for u in rows], 4) for k in range(4)]
            parts.append([jnp.concatenate([x[m] for x in by_k], axis=0) for m in range(len(rows))])
        for m, u in enumerate(rows):
            form([parts[c][m] for c in range(chunks)], wu, u, first + u)

    def codes(t, d, q):
        _, crow, shift = pay_row(pair * t + q)
        packed = pay[pl.ds(d * PAY + crow, 1), :].astype(I32)
        return (packed >> shift) & (PACK - 1)

    def by_lanes(t, d, q):
        code = jnp.broadcast_to(codes(t, d, q), (F, LN)).astype(I16)
        low = code & I16(LN - 1)
        head = code >> I16(7)
        acc = jnp.zeros((F, LN), BF16)
        for h in range(heads):
            acc = jnp.where(head == I16(h), take(tab[d, h], low, 1), acc)
        return acc

    def by_matmul(t, d):
        hots, halves = [], []
        for q in range(2):
            code = codes(t, d, q)
            low = (jnp.broadcast_to(code, (2 * LN, LN)) & (2 * LN - 1)).astype(I16)
            hots.append(jnp.where(low == ids[...], jnp.ones((2 * LN, LN), BF16), jnp.zeros((2 * LN, LN), BF16)))
            halves.append(jnp.broadcast_to(code, (F, LN)) >> 8)
        table = jnp.concatenate([jnp.concatenate([tab[d, 2 * h], tab[d, 2 * h + 1]], axis=1)
                                 for h in range(heads // 2)], axis=0)
        found = jnp.dot(table, jnp.concatenate(hots, axis=1), preferred_element_type=F32)
        out = []
        for q in range(2):
            acc = jnp.zeros((F, LN), F32)
            for h in range(heads // 2):
                acc = jnp.where(halves[q] == h, found[h * F:(h + 1) * F, q * LN:(q + 1) * LN], acc)
            out.append(acc.astype(BF16))
        return out

    def lookup(t, i, yu):
        turn = 0
        for quad in range(4):
            found = []
            for dd in range(4):
                d = 16 * i + 4 * quad + dd
                turn += lanes_of
                if turn >= 16:
                    turn -= 16
                    found.append([by_lanes(t, d, q) for q in range(pair)])
                else:
                    found.append(by_matmul(t, d))
            for q in range(pair):
                for k in range(4):
                    rows = slice(16 * k, 16 * k + 16)
                    xs = exchange([x[q][rows] for x in found], 1)
                    for a in range(4):
                        if slots == 8:
                            yu[16 * q + 4 * quad + a, i, rows, :] = xs[a]
                        else:
                            yu[64 * q + (i % 4) * 16 + 4 * quad + a, i // 4, rows, :] = xs[a]

    def flip(block, b):
        m = a_scr[pl.ds(block % 2 * (LN * PITCH) + b, LN, stride=PITCH), :].T
        at_scr[b] = m[:F]
        s_scr[pl.ds(b, 1), :] = m[F:F + 1]

    def flip_all(block):
        def four(b4, _):
            for e in range(4):
                flip(block, 4 * b4 + e)
            return 0

        lax.fori_loop(0, F // 4, four, 0)

    def solve(block):
        rhs = a_scr[pl.ds(block % 2 * (LN * PITCH) + F, LN, stride=PITCH), :].T[:F] + s_scr[...]
        x = x0_ref[:, pl.ds(pl.multiple_of(block * LN, LN), LN)]

        def apply_mat(vec):
            p_scr[...] = vec

            def add(b, acc):
                return acc + at_scr[b] * p_scr[pl.ds(b, 1), :]

            return lax.fori_loop(0, F, add, jnp.zeros((F, LN), F32), unroll=16)

        res = rhs - apply_mat(x)
        direction = res
        res_sq = jnp.sum(res * res, axis=0, keepdims=True)
        for step in range(CG_STEPS):
            q = apply_mat(direction)
            length = res_sq / jnp.sum(direction * q, axis=0, keepdims=True)
            x = x + length * direction
            if step + 1 < CG_STEPS:
                res = res - length * q
                new_sq = jnp.sum(res * res, axis=0, keepdims=True)
                direction = res + (new_sq / res_sq) * direction
                res_sq = new_sq
        out_ref[:, pl.ds(pl.multiple_of(block * LN, LN), LN)] = x
        if emit:
            xb = x.astype(BF16)
            tab_ref[block] = xb
            gout_ref[...] += fold(dot_nt(xb, xb))

    if emit:
        gout_ref[...] = jnp.zeros((F // 2, LN), F32)

    def weights(t, wu):
        for q in range(pair):
            spread_weights(pair * t + q, wu, q)

    def first_pass():
        weights(0, wu_a)

        def inner(i, _):
            tab_copy(i).wait()
            lookup(0, i, yu_a)
            return 0

        lax.fori_loop(0, 8, inner, 0)

    def step_pass(t, ahead, count, size, yu, wu, yu_last, wu_last):
        before = jnp.maximum((t - 1) // turns - 1, 0)
        if ahead:
            weights(jnp.minimum(t, steps - 1), wu)

        def inner(i2, _):
            flips = F // (8 * turns)
            for i in range(size):
                i = size * i2 + i
                for e in range(flips):
                    flip(before, ((t - 1) % turns * 8 + i) * flips + e)
                jobs = [functools.partial(form_rows, t, i, yu_last, wu_last)]
                if ahead:
                    jobs.insert(0 if body > 1 else 1, functools.partial(lookup, t, i, yu))
                for job in jobs:
                    job()
            return 0

        lax.fori_loop(0, count, inner, 0)

        def finish_block():
            @pl.when((t >= turns + 1) & (t % turns == 0))
            def _():
                solve(t // turns - 2)

        if ahead:
            pl.when(t < steps)(finish_block)
        else:
            finish_block()

    def two_steps(j, _):
        step_pass(2 * j + 1, True, 8 // body, body, yu_b, wu_b, yu_a, wu_a)
        step_pass(2 * j + 2, True, jnp.where(2 * j + 2 < steps, 8 // body, 0), body, yu_a, wu_a, yu_b, wu_b)
        return 0

    first_pass()
    lax.fori_loop(0, steps // 2, two_steps, 0)
    step_pass(steps, False, 8, 1, None, None, yu_b, wu_b)
    flip_all(blocks - 1)
    solve(blocks - 1)


def half_step(slots, emit, pair, lanes_of, body, tables, payload, gram, x0_t):
    n = x0_t.shape[1]
    heads = tables.shape[1]
    per = LN // slots
    chunks = G // per
    out_shape = [jax.ShapeDtypeStruct((F, n), F32)]
    if emit:
        out_shape += [jax.ShapeDtypeStruct((n // LN, F, LN), BF16), jax.ShapeDtypeStruct((F // 2, LN), F32)]
    vmem = pl.BlockSpec(memory_space=pltpu.VMEM)
    return pl.pallas_call(
        functools.partial(half_kernel, slots, n // LN, pair, lanes_of, body, emit),
        in_specs=[pl.BlockSpec(memory_space=pl.ANY), pl.BlockSpec(memory_space=pl.ANY), vmem, vmem],
        out_specs=[vmem] * len(out_shape),
        out_shape=out_shape,
        scratch_shapes=[
            pltpu.VMEM((G, heads, F, LN), BF16),
            pltpu.VMEM((G * PAY, LN), F32),
            pltpu.VMEM((2 * LN, LN), I16),
            pltpu.VMEM((pair * per, chunks, F, LN), BF16),
            pltpu.VMEM((pair * per, chunks, F, LN), BF16),
            pltpu.VMEM((chunks, pair * per, LN), F32),
            pltpu.VMEM((chunks, pair * per, LN), F32),
            pltpu.VMEM((2 * LN * PITCH, LN), F32),
            pltpu.VMEM((F, F, LN), F32),
            pltpu.VMEM((F, LN), F32),
            pltpu.VMEM((F, LN), F32),
            pltpu.SemaphoreType.DMA((9,)),
        ],
        compiler_params=pltpu.CompilerParams(vmem_limit_bytes=62 * 1024 * 1024),
        cost_estimate=pl.CostEstimate(flops=10 ** 11, bytes_accessed=2 ** 25, transcendentals=0),
        name='half_step',
    )(tables, payload, gram, x0_t)


def solution(mesh):
    part_spec = P(('tables', 'g'), None)
    slot_spec = P(('tables', 'g'), None, None)

    def local_sweep(item_block, start_block, item_idx, item_conf, user_idx, user_conf):
        item_t = item_block.T

        def as_rows(x):
            return x[0].reshape(-1, LN, 2).transpose(0, 2, 1).reshape(-1, LN)

        gram_shape = jax.ShapeDtypeStruct((F // 2, LN), F32)
        tables, gram_items, payload, late = gather_all(
            (item_t,), (jax.ShapeDtypeStruct((item_t.size // LN, LN), BF16), gram_shape), 0,
            (item_idx[0].T, item_conf[0].T, as_rows(user_idx), as_rows(user_conf)))
        late = lax.all_to_all(late, 'g', 0, 0, tiled=True)
        user_t, user_table, gram_part = half_step(8, True, 2, 6, 2, tables, payload.reshape(G * PAY, LN),
                                                  gram_items, start_block.T)
        user_table = user_table.reshape(-1, LN)
        user_tables, gram_users = gather_all((user_table, gram_part), (user_table, gram_part), 1)
        item_new = half_step(2, False, 2, 6, 1, user_tables, late.reshape(G * PAY, LN), gram_users, item_t)[0]
        return user_t.T, item_new.T

    return jax.shard_map(local_sweep, mesh=mesh,
                         in_specs=(part_spec, part_spec, slot_spec, slot_spec, slot_spec, slot_spec),
                         out_specs=(part_spec, part_spec), check_vma=False)
```

```python
import functools

import jax
import jax.numpy as jnp
from jax import lax
from jax.experimental import pallas as pl
from jax.experimental.pallas import tpu as pltpu
from jax.sharding import PartitionSpec as P


REG_LAMBDA = 0.01
CG_STEPS = 3
F = 64
FX = F + 16
PITCH = F + 8
LN = 128
G = 128
PAY = 48
EMPTY = 2048
PACK = 4096
F32 = jnp.float32
BF16 = jnp.bfloat16
I16 = jnp.int16
I32 = jnp.int32


def iota(shape, dim, dtype=I32):
    return lax.broadcasted_iota(dtype, shape, dim)


def take(x, ind, axis):
    other = 1 - axis
    dims = lax.GatherDimensionNumbers(
        offset_dims=(), collapsed_slice_dims=(axis,), start_index_map=(axis,),
        operand_batching_dims=(other,), start_indices_batching_dims=(other,))
    return lax.gather(x, ind[..., None], dims, slice_sizes=(1, 1),
                      mode=lax.GatherScatterMode.PROMISE_IN_BOUNDS)


def dot_nt(a, b):
    return lax.dot_general(a, b, (((1,), (1,)), ((), ())), preferred_element_type=F32)


def fold(gram):
    return jnp.concatenate([gram[:F // 2], gram[F // 2:]], axis=1)


def unfold(gram):
    return jnp.concatenate([gram[:, :F], gram[:, F:]], axis=0)


def make_table(x_ref, tab_ref, gram_ref):
    x = x_ref[...].astype(BF16)
    for h in range(x.shape[1] // LN):
        tab_ref[h * F:(h + 1) * F, :] = x[:, h * LN:(h + 1) * LN]
    gram_ref[...] = fold(dot_nt(x, x))


def code_weight(idx, conf):
    code = jnp.where(conf > 0.0, idx, EMPTY).astype(F32)
    return code, jnp.maximum(conf - 1.0, 0.0)


def arrange_users(me, idx_ref, conf_ref, out_ref, begin=0, end=None):
    skew = me % 16
    row, lane = iota((8, LN), 0), iota((8, LN), 1)
    first = (lane - 16 * row) & 127
    second = ((lane >> 4) - row) & 7
    third = ((lane ^ skew) + 16 * row) & 127
    dests = idx_ref.shape[1] // 512
    batch = min(8, dests)

    def arrange(x):
        return take(take(take(x, first, 1), second, 0), third, 1)

    def place(n, _):
        for e in range(batch):
            dest = n * batch + e
            owner = (dest // 32, dest // 8 % 4, dest // 2 % 4, dest % 2)
            codes = []
            for q in range(4):
                cols = pl.ds(pl.multiple_of(dest * 512 + q * LN, LN), LN)
                code, weight = code_weight(idx_ref[:, cols], conf_ref[:, cols])
                out_ref[(*owner, pl.ds(q * 8, 8), slice(None))] = arrange(weight)
                codes.append(arrange(code))
            for q in range(2):
                out_ref[(*owner, pl.ds(32 + q * 8, 8), slice(None))] = codes[q] + PACK * codes[q + 2]
        return 0

    lax.fori_loop(begin, dests // batch if end is None else end, place, 0)


def arrange_items(me, idx_ref, conf_ref, out_ref):
    skew = me % 64
    lane = iota((8, LN), 1)
    pattern = lane ^ skew
    low = lane < 64

    def halves(x0, x1):
        a = jnp.where(low, x0, pltpu.roll(x1, 64, 1))
        b = jnp.where(low, pltpu.roll(x0, 64, 1), x1)
        return take(a, pattern, 1), take(b, pattern, 1)

    def place(dest, _):
        for q in range(2):
            base = dest * 32 + q * 16
            rows = [pl.ds(base + j, 8, stride=2) for j in range(2)]
            pairs = [code_weight(idx_ref[r, :], conf_ref[r, :]) for r in rows]
            code_a, code_b = halves(pairs[0][0], pairs[1][0])
            weight_a, weight_b = halves(pairs[0][1], pairs[1][1])
            out_ref[dest, pl.ds(q * 8, 8), :] = weight_a
            out_ref[dest, pl.ds(16 + q * 8, 8), :] = weight_b
            out_ref[dest, pl.ds(32 + q * 8, 8), :] = code_a + PACK * code_b
        return 0

    lax.fori_loop(0, out_ref.shape[0], place, 0, unroll=min(8, out_ref.shape[0]))


ORDERS = ((2, 1, 0), (1, 0, 2), (0, 2, 1))
STRIDES = (32, 8, 2)
RING = 4


def gather_kernel(streams, beside_work, *refs):
    if beside_work:
        (rows_hbm, uidx_hbm, uconf_hbm, idx_hbm, conf_hbm, *outs, arrived, pay_hbm,
         send, recv, pass_send, pass_recv, local, uidx, uconf, idx, conf, pay, stage, relay,
         swap_send, swap_recv, work, table, gram, rows_ref) = refs
        loads = [pltpu.make_async_copy(a, b, work.at[n]) for n, (a, b) in enumerate(
            ((uidx_hbm, uidx), (uconf_hbm, uconf), (idx_hbm, idx), (conf_hbm, conf)))]
        firsts = [pltpu.make_async_copy(rows_hbm, rows_ref, work.at[6])]
    else:
        table_hbm, gram_hbm, *outs, send, recv, pass_send, pass_recv, local, table, gram, work = refs
        loads = []
        firsts = [pltpu.make_async_copy(table_hbm, table, work.at[0]), pltpu.make_async_copy(gram_hbm, gram, work.at[1])]
    for copy in firsts + loads:
        copy.start()
    ins = (table, gram)
    me = lax.axis_index('g')
    core = me % 2
    here = [me // stride % RING for stride in STRIDES]
    partner = me + 1 - 2 * core

    def beside(dim, delta):
        return me + ((here[dim] + delta + RING) % RING - here[dim]) * STRIDES[dim]

    barrier = pltpu.get_barrier_semaphore()
    peers = [beside(dim, delta) for dim in range(3) for delta in ((1, -1) if beside_work else (1, -1, 2))] + [partner]
    for peer in peers:
        pl.semaphore_signal(barrier, inc=1, device_id={'g': peer}, device_id_type=pl.DeviceIdType.MESH)
    for copy in firsts:
        copy.wait()
    if beside_work:
        make_table(rows_ref, table, gram)
    pl.semaphore_wait(barrier, len(peers))

    def region(s, phase, dim, delta, half):
        which, first, rows = streams[s][:3]
        order = ORDERS[streams[s][3]]
        index = []
        for d in range(3):
            if d in order[:phase]:
                index.append(pl.ds(0, RING))
            else:
                index.append((here[d] + delta + RING) % RING if d == dim else here[d])
        if half is not None:
            rows = rows // 2
            first = first + half * rows
        return outs[which].at[(*index, core, pl.ds(first, rows), slice(None))]

    def remote(src, dst, sems, index, peer):
        return pltpu.make_async_remote_copy(
            src_ref=src, dst_ref=dst, send_sem=sems[0].at[index], recv_sem=sems[1].at[index],
            device_id={'g': peer}, device_id_type=pl.DeviceIdType.MESH)

    swaps = {}

    def slab(level, dim, delta, color, half=None):
        index = [pl.ds(0, RING)] * 3
        index[dim] = (here[dim] + delta + RING) % RING
        rows = pl.ds(16 * color, 16) if half is None else pl.ds(16 * color + 8 * half, 8)
        return stage.at[(level, *index, pl.ds(0, 2), rows, slice(None))]

    def swap(src, dst, index, peer):
        copy = remote(src, dst, (swap_send, swap_recv), index, peer)
        copy.start()
        swaps[index] = copy

    def swap_start(phase):
        for color in range(3):
            dim = ORDERS[color][phase]
            base = (phase * 3 + color) * 6
            for way, delta in enumerate((1, -1)):
                swap(slab(phase, dim, delta, color), slab(phase + 1, dim, 0, color), base + way, beside(dim, delta))
                swap(slab(phase, dim, 2, color, way), relay.at[phase, color, way], base + 2 + way, beside(dim, delta))
        for color in range(3):
            dim = ORDERS[color][phase]
            index = [pl.ds(0, RING)] * 3
            index[dim] = pl.ds(here[dim], 1)
            part = (*index, pl.ds(0, 2), pl.ds(16 * color, 16), slice(None))
            stage[(phase + 1, *part)] = stage[(phase, *part)]

    def swap_further(phase):
        for color in range(3):
            dim = ORDERS[color][phase]
            base = (phase * 3 + color) * 6
            for way, delta in enumerate((1, -1)):
                swaps[base + 2 + way].wait_recv()
                swap(relay.at[phase, color, way], slab(phase + 1, dim, -delta, color, way), base + 4 + way, beside(dim, delta))

    def swap_finish(phase):
        for color in range(3):
            base = (phase * 3 + color) * 6
            for n in (0, 1, 4, 5):
                swaps[base + n].wait_recv()

    def swap_cores():
        everywhere = [pl.ds(0, RING)] * 3
        mine = arrived.at[(*everywhere, core)]
        swap(stage.at[(3, *everywhere, 1 - core)], mine, 54, partner)
        stay = pltpu.make_async_copy(stage.at[(3, *everywhere, core)], mine, work.at[4])
        stay.start()
        stay.wait()
        for copy in swaps.values():
            copy.wait_send()
        swaps[54].wait_recv()

    passed = {s: [] for s in range(len(streams))}

    def pass_on(src, dst, s, slot):
        copy = remote(src, dst, (pass_send, pass_recv), 13 * s + slot, partner)
        copy.start()
        passed[s].append(copy)

    count = len(streams)
    own, kept = [], []
    for s, (which, first, rows, _) in enumerate(streams):
        src = ins[which].at[pl.ds(first, rows), :]
        own.append(src)
        copy = pltpu.make_async_copy(src, region(s, 0, 0, 0, None), local.at[s])
        copy.start()
        kept.append(copy)
    sent, across, further = [], {}, {}

    def start_across(s, phase):
        dim = ORDERS[streams[s][3]][phase]
        for way, delta in enumerate((1, -1)):
            mine = region(s, phase, dim, 0, None)
            src = own[s] if phase == 0 else mine
            across[s, way] = remote(src, mine, (send, recv), ((s * 3 + phase) * 2 + 0) * 2 + way, beside(dim, delta))
            across[s, way].start()
            sent.append(across[s, way])
        if phase == 0 and not beside_work:
            opposite = remote(own[s], region(s, phase, dim, 0, None), (send, recv), (s * 3 * 2 + 1) * 2, beside(dim, 2))
            opposite.start()
            sent.append(opposite)
            further[s, 0] = opposite

    def start_further(s, phase):
        dim = ORDERS[streams[s][3]][phase]
        if phase == 0 and not beside_work:
            for way, delta in enumerate((1, -1)):
                across[s, way].wait_recv()
                whole = region(s, phase, dim, -delta, None)
                pass_on(whole, whole, s, 1 + way)
            return
        for way, delta in enumerate((1, -1)):
            across[s, way].wait_recv()
            half = region(s, phase, dim, -delta, way)
            further[s, way] = remote(half, half, (send, recv), ((s * 3 + phase) * 2 + 1) * 2 + way, beside(dim, delta))
            further[s, way].start()
            sent.append(further[s, way])
        for way, delta in enumerate((1, -1)):
            whole = region(s, phase, dim, -delta, None)
            pass_on(whole, whole, s, 1 + 4 * phase + way)

    def finish(s, phase):
        dim = ORDERS[streams[s][3]][phase]
        once = phase == 0 and not beside_work
        for way in range(1 if once else 2):
            further[s, way].wait_recv()
        if phase == 0:
            kept[s].wait()
        if phase < 2:
            start_across(s, phase + 1)
        for way in range(1 if once else 2):
            half = region(s, phase, dim, 2, None if once else way)
            pass_on(half, half, s, 3 + 4 * phase + way)

    for s in range(count):
        start_across(s, 0)
    for s in range(count):
        pass_on(own[s], region(s, 0, 0, 0, None), s, 0)

    def every(step, phase, part=slice(None)):
        for s in range(count)[part]:
            step(s, phase)

    early, late = slice(0, 4), slice(4, None)
    if beside_work:
        loads[0].wait()
        loads[1].wait()
        arrange_users(me, uidx, uconf, stage.at[0], 0, 8)
        every(start_further, 0)
        arrange_users(me, uidx, uconf, stage.at[0], 8, 16)
        every(finish, 0)
        swap_start(0)
        every(start_further, 1)
        every(finish, 1, early)
        swap_further(0)
        swap_finish(0)
        swap_start(1)
        every(finish, 1, late)
        loads[2].wait()
        loads[3].wait()
        arrange_items(me, idx, conf, pay)
        swap_further(1)
        swap_finish(1)
        swap_start(2)
        every(start_further, 2, early)
        store = pltpu.make_async_copy(pay, pay_hbm, work.at[5])
        store.start()
        swap_further(2)
        every(start_further, 2, late)
        swap_finish(2)
        every(finish, 2)
        swap_cores()
        store.wait()
    else:
        for phase in range(3):
            every(start_further, phase)
            every(finish, phase)
    for copy in sent:
        copy.wait_send()
    for s in range(count):
        for copy in passed[s]:
            copy.wait_send()
    for s in range(count):
        for copy in passed[s]:
            copy.wait_recv()


def gather_all(sources, shapes, collective_id, slots=()):
    table, gram = shapes
    rows = table.shape[0]
    units = rows // 16
    parts = 3 if slots else 2
    share = (units + 4) // 3
    totals = (share, share, units - 2 * share)
    sizes = [total // parts + (n < total % parts) for n in range(parts) for total in totals]
    streams, first = [(1, 0, gram.shape[0], 2)], 0
    for n, size in enumerate(sizes):
        streams.append((0, first, 16 * size, n % 3))
        first += 16 * size
    count = len(streams)
    any_spec = pl.BlockSpec(memory_space=pl.ANY)
    out_shape = [jax.ShapeDtypeStruct((RING, RING, RING, 2, *x.shape), x.dtype) for x in shapes]
    scratch = [pltpu.SemaphoreType.DMA((12 * count,)), pltpu.SemaphoreType.DMA((12 * count,)),
               pltpu.SemaphoreType.DMA((13 * count,)), pltpu.SemaphoreType.DMA((13 * count,)),
               pltpu.SemaphoreType.DMA((count,))]
    if slots:
        blocks = (RING, RING, RING, 2, PAY, LN)
        out_shape += [jax.ShapeDtypeStruct(blocks, F32), jax.ShapeDtypeStruct((G, PAY, LN), F32)]
        scratch += [pltpu.VMEM(x.shape, x.dtype) for x in slots]
        scratch += [pltpu.VMEM((G, PAY, LN), F32), pltpu.VMEM((4, *blocks), F32),
                    pltpu.VMEM((3, 3, 2, RING, RING, 2, 8, LN), F32),
                    pltpu.SemaphoreType.DMA((55,)), pltpu.SemaphoreType.DMA((55,)), pltpu.SemaphoreType.DMA((7,)),
                    pltpu.VMEM(table.shape, table.dtype), pltpu.VMEM(gram.shape, gram.dtype),
                    pltpu.VMEM(sources[0].shape, F32)]
    else:
        scratch += [pltpu.VMEM(table.shape, table.dtype), pltpu.VMEM(gram.shape, gram.dtype), pltpu.SemaphoreType.DMA((2,))]
    tables, grams, *payload = pl.pallas_call(
        functools.partial(gather_kernel, tuple(streams), bool(slots)),
        in_specs=[any_spec] * (len(sources) + len(slots)),
        out_specs=[any_spec] * len(out_shape),
        out_shape=out_shape,
        scratch_shapes=scratch,
        compiler_params=pltpu.CompilerParams(collective_id=collective_id, has_side_effects=True),
        name='gather_all',
    )(*sources, *slots)
    return tables.reshape(G, -1, F, LN), grams.reshape(-1, LN), *payload


def half_kernel(slots, blocks, pair, lanes_of, body, emit, tab_hbm, pay_hbm, gram_hbm, x0_hbm, *refs):
    if emit:
        out_ref, tab_ref, gout_ref = refs[:3]
        refs = refs[3:]
    else:
        out_ref = refs[0]
        refs = refs[1:]
    tab, pay, ids, yu_a, yu_b, wu_a, wu_b, a_scr, at_scr, p_scr, s_scr, gpad_ref, gram_ref, x0_ref, sems = refs
    per = LN // slots
    chunks = G // per
    groups = LN // per
    steps = blocks * groups // pair
    turns = groups // pair
    heads = tab.shape[1]

    pay_copy = pltpu.make_async_copy(pay_hbm, pay, sems.at[8])
    pay_copy.start()

    def tab_copy(i):
        return pltpu.make_async_copy(tab_hbm.at[pl.ds(16 * i, 16)], tab.at[pl.ds(16 * i, 16)], sems.at[i])

    for i in range(8):
        tab_copy(i).start()
    side_copies = [pltpu.make_async_copy(gram_hbm, gram_ref, sems.at[9]), pltpu.make_async_copy(x0_hbm, x0_ref, sems.at[10])]
    for copy in side_copies:
        copy.start()
    ids[...] = iota((2 * LN, LN), 0, I16)
    pay_copy.wait()

    lane16 = iota((16, LN), 1, I16)
    lane = iota((8, LN), 1)
    row = iota((8, LN), 0)

    def sum_grams():
        for copy in side_copies:
            copy.wait()

        def add_gram(d, acc):
            return acc + gram_ref[pl.ds(pl.multiple_of(d * (F // 2), F // 2), F // 2), :]

        gram = lax.fori_loop(0, G, add_gram, jnp.zeros((F // 2, LN), F32), unroll=8)
        gpad = jnp.concatenate([unfold(gram), jnp.zeros((16, F), F32)], axis=0)
        gpad = jnp.concatenate([gpad, jnp.zeros((FX, 16), F32)], axis=1)
        rr, cc = iota((FX, FX), 0), iota((FX, FX), 1)
        gpad_ref[...] = gpad + jnp.where((rr == cc) & (rr < F), REG_LAMBDA, 0.0)

    def pay_row(t):
        if slots == 8:
            return t, 32 + t % 16, 12 * (t // 16)
        return (t % 2) * 16 + t // 2, 32 + t // 2, 12 * (t % 2)

    def spread_weights(t, wu, q):
        wrow = pay_row(t)[0]
        for c in range(chunks):
            tiles = []
            for v in range(per // 8):
                start = (per * c + 8 * v) * PAY + wrow
                tiles.append(pay[pl.ds(start, 8, stride=PAY), :])
            for bit in (1, 2, 4):
                hit = (lane & bit) != 0
                up = (row & bit) != 0
                for v in range(len(tiles)):
                    x = tiles[v]
                    if bit == 4:
                        other = pltpu.roll(x, 4, 0)
                    else:
                        other = jnp.where(up, pltpu.roll(x, bit, 0), pltpu.roll(x, 8 - bit, 0))
                    tiles[v] = jnp.where(hit, other, x)
            bit = 8
            while bit < per:
                hit = (lane & bit) != 0
                tiles = [jnp.where(hit, tiles[v ^ (bit // 8)], tiles[v]) for v in range(len(tiles))]
                bit *= 2
            for v in range(len(tiles)):
                wu[c, pl.ds(per * q + 8 * v, 8), :] = tiles[v]

    def exchange(xs, low_bit):
        bit, n = 1, len(xs)
        while bit < n:
            hit = (lane16 & I16(bit * low_bit)) != I16(0)
            xs = [jnp.where(hit, xs[a ^ bit], xs[a]) for a in range(n)]
            bit *= 2
        return xs

    ones = jnp.ones((16, LN * chunks), BF16)

    def form(y_parts, wu, u, at):
        vs = []
        for c in range(chunks):
            w = wu[c, pl.ds(u, 1), :]
            vs.append((y_parts[c].astype(F32) * w).astype(BF16))
        y = jnp.concatenate([jnp.concatenate(y_parts, axis=1), ones], axis=0)
        v = jnp.concatenate([jnp.concatenate(vs, axis=1), ones], axis=0)
        a_scr[pl.ds(at * PITCH, PITCH), pl.ds(0, FX)] = (dot_nt(y, v) + gpad_ref[...])[:PITCH]

    def form_rows(t, i, yu, wu):
        first = (t - 1) // turns % 2 * LN + (t - 1) % turns * (per * pair)
        rows = [per * (i // 4) + i % 4 + 4 * m for m in range(per // 4)]
        parts = []
        for c in range(chunks):
            by_k = [exchange([yu[u, c, pl.ds(16 * k, 16), :] for u in rows], 4) for k in range(4)]
            parts.append([jnp.concatenate([x[m] for x in by_k], axis=0) for m in range(len(rows))])
        for m, u in enumerate(rows):
            form([parts[c][m] for c in range(chunks)], wu, u, first + u)

    def codes(t, d, q):
        _, crow, shift = pay_row(pair * t + q)
        packed = pay[pl.ds(d * PAY + crow, 1), :].astype(I32)
        return (packed >> shift) & (PACK - 1)

    def by_lanes(t, d, q):
        code = jnp.broadcast_to(codes(t, d, q), (F, LN)).astype(I16)
        low = code & I16(LN - 1)
        head = code >> I16(7)
        acc = jnp.zeros((F, LN), BF16)
        for h in range(heads):
            acc = jnp.where(head == I16(h), take(tab[d, h], low, 1), acc)
        return acc

    def by_matmul(t, d):
        hots, halves = [], []
        for q in range(2):
            code = codes(t, d, q)
            low = (jnp.broadcast_to(code, (2 * LN, LN)) & (2 * LN - 1)).astype(I16)
            hots.append(jnp.where(low == ids[...], jnp.ones((2 * LN, LN), BF16), jnp.zeros((2 * LN, LN), BF16)))
            halves.append(jnp.broadcast_to(code, (F, LN)) >> 8)
        table = jnp.concatenate([jnp.concatenate([tab[d, 2 * h], tab[d, 2 * h + 1]], axis=1)
                                 for h in range(heads // 2)], axis=0)
        found = jnp.dot(table, jnp.concatenate(hots, axis=1), preferred_element_type=F32)
        out = []
        for q in range(2):
            acc = jnp.zeros((F, LN), F32)
            for h in range(heads // 2):
                acc = jnp.where(halves[q] == h, found[h * F:(h + 1) * F, q * LN:(q + 1) * LN], acc)
            out.append(acc.astype(BF16))
        return out

    def lookup(t, i, yu):
        for quad in range(4):
            found = []
            for dd in range(4):
                d = 16 * i + 4 * quad + dd
                if 4 * quad + dd < lanes_of:
                    found.append([by_lanes(t, d, q) for q in range(pair)])
                else:
                    found.append(by_matmul(t, d))
            for q in range(pair):
                for k in range(4):
                    rows = slice(16 * k, 16 * k + 16)
                    xs = exchange([x[q][rows] for x in found], 1)
                    for a in range(4):
                        if slots == 8:
                            yu[16 * q + 4 * quad + a, i, rows, :] = xs[a]
                        else:
                            yu[64 * q + (i % 4) * 16 + 4 * quad + a, i // 4, rows, :] = xs[a]

    def flip(block, b):
        m = a_scr[pl.ds(block % 2 * (LN * PITCH) + b, LN, stride=PITCH), :].T
        at_scr[b] = m[:F]
        s_scr[pl.ds(b, 1), :] = m[F:F + 1]

    def flip_all(block):
        def four(b4, _):
            for e in range(4):
                flip(block, 4 * b4 + e)
            return 0

        lax.fori_loop(0, F // 4, four, 0)

    def solve(block):
        rhs = a_scr[pl.ds(block % 2 * (LN * PITCH) + F, LN, stride=PITCH), :].T[:F] + s_scr[...]
        x = x0_ref[:, pl.ds(pl.multiple_of(block * LN, LN), LN)]

        def apply_mat(vec):
            p_scr[...] = vec

            def add(b, acc):
                return acc + at_scr[b] * p_scr[pl.ds(b, 1), :]

            return lax.fori_loop(0, F, add, jnp.zeros((F, LN), F32), unroll=16)

        res = rhs - apply_mat(x)
        direction = res
        res_sq = jnp.sum(res * res, axis=0, keepdims=True)
        for step in range(CG_STEPS):
            q = apply_mat(direction)
            length = res_sq / jnp.sum(direction * q, axis=0, keepdims=True)
            x = x + length * direction
            if step + 1 < CG_STEPS:
                res = res - length * q
                new_sq = jnp.sum(res * res, axis=0, keepdims=True)
                direction = res + (new_sq / res_sq) * direction
                res_sq = new_sq
        out_ref[:, pl.ds(pl.multiple_of(block * LN, LN), LN)] = x
        if emit:
            xb = x.astype(BF16)
            tab_ref[block] = xb
            gout_ref[...] += fold(dot_nt(xb, xb))

    if emit:
        gout_ref[...] = jnp.zeros((F // 2, LN), F32)

    def weights(t, wu):
        for q in range(pair):
            spread_weights(pair * t + q, wu, q)

    def first_pass():
        weights(0, wu_a)

        def inner(i, _):
            tab_copy(i).wait()
            lookup(0, i, yu_a)
            return 0

        lax.fori_loop(0, 8, inner, 0)

    def step_pass(t, ahead, count, size, yu, wu, yu_last, wu_last):
        before = jnp.maximum((t - 1) // turns - 1, 0)
        if ahead:
            weights(jnp.minimum(t, steps - 1), wu)

        def inner(i2, _):
            flips = F // (8 * turns)
            for i in range(size):
                i = size * i2 + i
                for e in range(flips):
                    flip(before, ((t - 1) % turns * 8 + i) * flips + e)
                jobs = [functools.partial(form_rows, t, i, yu_last, wu_last)]
                if ahead:
                    jobs.insert(0 if body > 1 else 1, functools.partial(lookup, t, i, yu))
                for job in jobs:
                    job()
            return 0

        lax.fori_loop(0, count, inner, 0)

        def finish_block():
            @pl.when((t >= turns + 1) & (t % turns == 0))
            def _():
                solve(t // turns - 2)

        if ahead:
            pl.when(t < steps)(finish_block)
        else:
            finish_block()

    def two_steps(j, _):
        step_pass(2 * j + 1, True, 8 // body, body, yu_b, wu_b, yu_a, wu_a)
        step_pass(2 * j + 2, True, jnp.where(2 * j + 2 < steps, 8 // body, 0), body, yu_a, wu_a, yu_b, wu_b)
        return 0

    first_pass()
    sum_grams()
    lax.fori_loop(0, steps // 2, two_steps, 0)
    step_pass(steps, False, 8, 1, None, None, yu_b, wu_b)
    flip_all(blocks - 1)
    solve(blocks - 1)


def half_step(slots, emit, pair, lanes_of, body, tables, payload, gram, x0_t):
    n = x0_t.shape[1]
    heads = tables.shape[1]
    per = LN // slots
    chunks = G // per
    out_shape = [jax.ShapeDtypeStruct((F, n), F32)]
    if emit:
        out_shape += [jax.ShapeDtypeStruct((n // LN, F, LN), BF16), jax.ShapeDtypeStruct((F // 2, LN), F32)]
    vmem = pl.BlockSpec(memory_space=pltpu.VMEM)
    return pl.pallas_call(
        functools.partial(half_kernel, slots, n // LN, pair, lanes_of, body, emit),
        in_specs=[pl.BlockSpec(memory_space=pl.ANY)] * 4,
        out_specs=[vmem] * len(out_shape),
        out_shape=out_shape,
        scratch_shapes=[
            pltpu.VMEM((G, heads, F, LN), BF16),
            pltpu.VMEM((G * PAY, LN), F32),
            pltpu.VMEM((2 * LN, LN), I16),
            pltpu.VMEM((pair * per, chunks, F, LN), BF16),
            pltpu.VMEM((pair * per, chunks, F, LN), BF16),
            pltpu.VMEM((chunks, pair * per, LN), F32),
            pltpu.VMEM((chunks, pair * per, LN), F32),
            pltpu.VMEM((2 * LN * PITCH, LN), F32),
            pltpu.VMEM((F, F, LN), F32),
            pltpu.VMEM((F, LN), F32),
            pltpu.VMEM((F, LN), F32),
            pltpu.VMEM((FX, FX), F32),
            pltpu.VMEM(gram.shape, F32),
            pltpu.VMEM(x0_t.shape, F32),
            pltpu.SemaphoreType.DMA((11,)),
        ],
        compiler_params=pltpu.CompilerParams(vmem_limit_bytes=62 * 1024 * 1024),
        cost_estimate=pl.CostEstimate(flops=10 ** 11, bytes_accessed=2 ** 25, transcendentals=0),
        name='half_step',
    )(tables, payload, gram, x0_t)


def solution(mesh):
    part_spec = P(('tables', 'g'), None)
    slot_spec = P(('tables', 'g'), None, None)

    def local_sweep(item_block, start_block, item_idx, item_conf, user_idx, user_conf):
        item_t = item_block.T

        def as_rows(x):
            return x[0].reshape(-1, LN, 2).transpose(0, 2, 1).reshape(-1, LN)

        gram_shape = jax.ShapeDtypeStruct((F // 2, LN), F32)
        tables, gram_items, payload, late = gather_all(
            (item_t,), (jax.ShapeDtypeStruct((item_t.size // LN, LN), BF16), gram_shape), 0,
            (item_idx[0].T, item_conf[0].T, as_rows(user_idx), as_rows(user_conf)))
        late = lax.all_to_all(late, 'g', 0, 0, tiled=True)
        user_t, user_table, gram_part = half_step(8, True, 2, 6, 2, tables, payload.reshape(G * PAY, LN),
                                                  gram_items, start_block.T)
        user_table = user_table.reshape(-1, LN)
        user_tables, gram_users = gather_all((user_table, gram_part), (user_table, gram_part), 1)
        item_new = half_step(2, False, 2, 6, 1, user_tables, late.reshape(G * PAY, LN), gram_users, item_t)[0]
        return user_t.T, item_new.T

    return jax.shard_map(local_sweep, mesh=mesh,
                         in_specs=(part_spec, part_spec, slot_spec, slot_spec, slot_spec, slot_spec),
                         out_specs=(part_spec, part_spec), check_vma=False)
```

```python
import functools

import jax
import jax.numpy as jnp
from jax import lax
from jax.experimental import pallas as pl
from jax.experimental.pallas import tpu as pltpu
from jax.sharding import PartitionSpec as P


REG_LAMBDA = 0.01
CG_STEPS = 3
F = 64
FX = F + 16
PITCH = F + 8
LN = 128
G = 128
PAY = 48
EMPTY = 2048
PACK = 4096
F32 = jnp.float32
BF16 = jnp.bfloat16
I16 = jnp.int16
I32 = jnp.int32


def iota(shape, dim, dtype=I32):
    return lax.broadcasted_iota(dtype, shape, dim)


def take(x, ind, axis):
    other = 1 - axis
    dims = lax.GatherDimensionNumbers(
        offset_dims=(), collapsed_slice_dims=(axis,), start_index_map=(axis,),
        operand_batching_dims=(other,), start_indices_batching_dims=(other,))
    return lax.gather(x, ind[..., None], dims, slice_sizes=(1, 1),
                      mode=lax.GatherScatterMode.PROMISE_IN_BOUNDS)


def dot_nt(a, b):
    return lax.dot_general(a, b, (((1,), (1,)), ((), ())), preferred_element_type=F32)


def fold(gram):
    return jnp.concatenate([gram[:F // 2], gram[F // 2:]], axis=1)


def unfold(gram):
    return jnp.concatenate([gram[:, :F], gram[:, F:]], axis=0)


def make_table(x_ref, tab_ref, gram_ref):
    x = x_ref[...].astype(BF16)
    for h in range(x.shape[1] // LN):
        tab_ref[h * F:(h + 1) * F, :] = x[:, h * LN:(h + 1) * LN]
    gram_ref[...] = fold(dot_nt(x, x))


def code_weight(idx, conf):
    code = jnp.where(conf > 0.0, idx, EMPTY).astype(F32)
    return code, jnp.maximum(conf - 1.0, 0.0)


def arrange_users(me, idx_ref, conf_ref, out_ref, begin=0, end=None):
    skew = me % 16
    row, lane = iota((8, LN), 0), iota((8, LN), 1)
    first = (lane - 16 * row) & 127
    second = ((lane >> 4) - row) & 7
    third = ((lane ^ skew) + 16 * row) & 127
    dests = idx_ref.shape[1] // 512
    batch = min(8, dests)

    def arrange(x):
        return take(take(take(x, first, 1), second, 0), third, 1)

    def place(n, _):
        for e in range(batch):
            dest = n * batch + e
            owner = (dest // 32, dest // 8 % 4, dest // 2 % 4, dest % 2)
            codes = []
            for q in range(4):
                cols = pl.ds(pl.multiple_of(dest * 512 + q * LN, LN), LN)
                code, weight = code_weight(idx_ref[:, cols], conf_ref[:, cols])
                out_ref[(*owner, pl.ds(q * 8, 8), slice(None))] = arrange(weight)
                codes.append(arrange(code))
            for q in range(2):
                out_ref[(*owner, pl.ds(32 + q * 8, 8), slice(None))] = codes[q] + PACK * codes[q + 2]
        return 0

    lax.fori_loop(begin, dests // batch if end is None else end, place, 0)


def arrange_items(me, idx_ref, conf_ref, out_ref):
    skew = me % 64
    lane = iota((8, LN), 1)
    pattern = lane ^ skew
    low = lane < 64

    def halves(x0, x1):
        a = jnp.where(low, x0, pltpu.roll(x1, 64, 1))
        b = jnp.where(low, pltpu.roll(x0, 64, 1), x1)
        return take(a, pattern, 1), take(b, pattern, 1)

    def place(dest, _):
        for q in range(2):
            base = dest * 32 + q * 16
            rows = [pl.ds(base + j, 8, stride=2) for j in range(2)]
            pairs = [code_weight(idx_ref[r, :], conf_ref[r, :]) for r in rows]
            code_a, code_b = halves(pairs[0][0], pairs[1][0])
            weight_a, weight_b = halves(pairs[0][1], pairs[1][1])
            out_ref[dest, pl.ds(q * 8, 8), :] = weight_a
            out_ref[dest, pl.ds(16 + q * 8, 8), :] = weight_b
            out_ref[dest, pl.ds(32 + q * 8, 8), :] = code_a + PACK * code_b
        return 0

    lax.fori_loop(0, out_ref.shape[0], place, 0, unroll=min(8, out_ref.shape[0]))


ORDERS = ((2, 1, 0), (1, 0, 2), (0, 2, 1))
STRIDES = (32, 8, 2)
RING = 4


def gather_kernel(streams, beside_work, *refs):
    if beside_work:
        (rows_hbm, uidx_hbm, uconf_hbm, idx_hbm, conf_hbm, *outs, arrived, pay_hbm,
         send, recv, pass_send, pass_recv, local, uidx, uconf, idx, conf, pay, stage, relay,
         swap_send, swap_recv, work, table, gram, rows_ref) = refs
        loads = [pltpu.make_async_copy(a, b, work.at[n]) for n, (a, b) in enumerate(
            ((uidx_hbm, uidx), (uconf_hbm, uconf), (idx_hbm, idx), (conf_hbm, conf)))]
        firsts = [pltpu.make_async_copy(rows_hbm, rows_ref, work.at[6])]
    else:
        table_hbm, gram_hbm, *outs, send, recv, pass_send, pass_recv, local, table, gram, work = refs
        loads = []
        firsts = [pltpu.make_async_copy(table_hbm, table, work.at[0]), pltpu.make_async_copy(gram_hbm, gram, work.at[1])]
    for copy in firsts + loads:
        copy.start()
    ins = (table, gram)
    me = lax.axis_index('g')
    core = me % 2
    here = [me // stride % RING for stride in STRIDES]
    partner = me + 1 - 2 * core

    def beside(dim, delta):
        return me + ((here[dim] + delta + RING) % RING - here[dim]) * STRIDES[dim]

    barrier = pltpu.get_barrier_semaphore()
    peers = [beside(dim, delta) for dim in range(3) for delta in ((1, -1) if beside_work else (1, -1, 2))] + [partner]
    for peer in peers:
        pl.semaphore_signal(barrier, inc=1, device_id={'g': peer}, device_id_type=pl.DeviceIdType.MESH)
    for copy in firsts:
        copy.wait()
    if beside_work:
        make_table(rows_ref, table, gram)
    pl.semaphore_wait(barrier, len(peers))

    def region(s, phase, dim, delta, half):
        which, first, rows = streams[s][:3]
        order = ORDERS[streams[s][3]]
        index = []
        for d in range(3):
            if d in order[:phase]:
                index.append(pl.ds(0, RING))
            else:
                index.append((here[d] + delta + RING) % RING if d == dim else here[d])
        if half is not None:
            rows = rows // 2
            first = first + half * rows
        return outs[which].at[(*index, core, pl.ds(first, rows), slice(None))]

    def remote(src, dst, sems, index, peer):
        return pltpu.make_async_remote_copy(
            src_ref=src, dst_ref=dst, send_sem=sems[0].at[index], recv_sem=sems[1].at[index],
            device_id={'g': peer}, device_id_type=pl.DeviceIdType.MESH)

    swaps = {}

    def slab(level, dim, delta, color, half=None):
        index = [pl.ds(0, RING)] * 3
        index[dim] = (here[dim] + delta + RING) % RING
        rows = pl.ds(16 * color, 16) if half is None else pl.ds(16 * color + 8 * half, 8)
        return stage.at[(level, *index, pl.ds(0, 2), rows, slice(None))]

    def swap(src, dst, index, peer):
        copy = remote(src, dst, (swap_send, swap_recv), index, peer)
        copy.start()
        swaps[index] = copy

    def swap_start(phase):
        for color in range(3):
            dim = ORDERS[color][phase]
            base = (phase * 3 + color) * 6
            for way, delta in enumerate((1, -1)):
                swap(slab(phase, dim, delta, color), slab(phase + 1, dim, 0, color), base + way, beside(dim, delta))
                swap(slab(phase, dim, 2, color, way), relay.at[phase, color, way], base + 2 + way, beside(dim, delta))
        for color in range(3):
            dim = ORDERS[color][phase]
            index = [pl.ds(0, RING)] * 3
            index[dim] = pl.ds(here[dim], 1)
            part = (*index, pl.ds(0, 2), pl.ds(16 * color, 16), slice(None))
            stage[(phase + 1, *part)] = stage[(phase, *part)]

    def swap_further(phase):
        for color in range(3):
            dim = ORDERS[color][phase]
            base = (phase * 3 + color) * 6
            for way, delta in enumerate((1, -1)):
                swaps[base + 2 + way].wait_recv()
                swap(relay.at[phase, color, way], slab(phase + 1, dim, -delta, color, way), base + 4 + way, beside(dim, delta))

    def swap_finish(phase):
        for color in range(3):
            base = (phase * 3 + color) * 6
            for n in (0, 1, 4, 5):
                swaps[base + n].wait_recv()

    def swap_cores():
        everywhere = [pl.ds(0, RING)] * 3
        mine = arrived.at[(*everywhere, core)]
        swap(stage.at[(3, *everywhere, 1 - core)], mine, 54, partner)
        stay = pltpu.make_async_copy(stage.at[(3, *everywhere, core)], mine, work.at[4])
        stay.start()
        stay.wait()
        for copy in swaps.values():
            copy.wait_send()
        swaps[54].wait_recv()

    passed = {s: [] for s in range(len(streams))}

    def pass_on(src, dst, s, slot):
        copy = remote(src, dst, (pass_send, pass_recv), 13 * s + slot, partner)
        copy.start()
        passed[s].append(copy)

    count = len(streams)
    own, kept = [], []
    for s, (which, first, rows, _) in enumerate(streams):
        src = ins[which].at[pl.ds(first, rows), :]
        own.append(src)
        copy = pltpu.make_async_copy(src, region(s, 0, 0, 0, None), local.at[s])
        copy.start()
        kept.append(copy)
    sent, across, further = [], {}, {}

    def start_across(s, phase):
        dim = ORDERS[streams[s][3]][phase]
        for way, delta in enumerate((1, -1)):
            mine = region(s, phase, dim, 0, None)
            src = own[s] if phase == 0 else mine
            across[s, way] = remote(src, mine, (send, recv), ((s * 3 + phase) * 2 + 0) * 2 + way, beside(dim, delta))
            across[s, way].start()
            sent.append(across[s, way])
        if phase == 0 and not beside_work:
            opposite = remote(own[s], region(s, phase, dim, 0, None), (send, recv), (s * 3 * 2 + 1) * 2, beside(dim, 2))
            opposite.start()
            sent.append(opposite)
            further[s, 0] = opposite

    def start_further(s, phase):
        dim = ORDERS[streams[s][3]][phase]
        if phase == 0 and not beside_work:
            for way, delta in enumerate((1, -1)):
                across[s, way].wait_recv()
                whole = region(s, phase, dim, -delta, None)
                pass_on(whole, whole, s, 1 + way)
            return
        for way, delta in enumerate((1, -1)):
            across[s, way].wait_recv()
            half = region(s, phase, dim, -delta, way)
            further[s, way] = remote(half, half, (send, recv), ((s * 3 + phase) * 2 + 1) * 2 + way, beside(dim, delta))
            further[s, way].start()
            sent.append(further[s, way])
        for way, delta in enumerate((1, -1)):
            whole = region(s, phase, dim, -delta, None)
            pass_on(whole, whole, s, 1 + 4 * phase + way)

    def finish(s, phase):
        dim = ORDERS[streams[s][3]][phase]
        once = phase == 0 and not beside_work
        for way in range(1 if once else 2):
            further[s, way].wait_recv()
        if phase == 0:
            kept[s].wait()
        if phase < 2:
            start_across(s, phase + 1)
        for way in range(1 if once else 2):
            half = region(s, phase, dim, 2, None if once else way)
            pass_on(half, half, s, 3 + 4 * phase + way)

    for s in range(count):
        start_across(s, 0)
    for s in range(count):
        pass_on(own[s], region(s, 0, 0, 0, None), s, 0)

    def every(step, phase, part=slice(None)):
        for s in range(count)[part]:
            step(s, phase)

    early, late = slice(0, 4), slice(4, None)
    if beside_work:
        loads[0].wait()
        loads[1].wait()
        arrange_users(me, uidx, uconf, stage.at[0], 0, 8)
        every(start_further, 0)
        arrange_users(me, uidx, uconf, stage.at[0], 8, 16)
        every(finish, 0)
        swap_start(0)
        every(start_further, 1)
        every(finish, 1, early)
        swap_further(0)
        swap_finish(0)
        swap_start(1)
        every(finish, 1, late)
        loads[2].wait()
        loads[3].wait()
        arrange_items(me, idx, conf, pay)
        swap_further(1)
        swap_finish(1)
        swap_start(2)
        every(start_further, 2, early)
        store = pltpu.make_async_copy(pay, pay_hbm, work.at[5])
        store.start()
        swap_further(2)
        every(start_further, 2, late)
        swap_finish(2)
        every(finish, 2)
        swap_cores()
        store.wait()
    else:
        for phase in range(3):
            every(start_further, phase)
            every(finish, phase)
    for copy in sent:
        copy.wait_send()
    for s in range(count):
        for copy in passed[s]:
            copy.wait_send()
    for s in range(count):
        for copy in passed[s]:
            copy.wait_recv()


def gather_all(sources, shapes, collective_id, slots=()):
    table, gram = shapes
    rows = table.shape[0]
    units = rows // 16
    parts = 3 if slots else 2
    share = (units + 4) // 3
    totals = (share, share, units - 2 * share)
    sizes = [total // parts + (n < total % parts) for n in range(parts) for total in totals]
    streams, first = [(1, 0, gram.shape[0], 2)], 0
    for n, size in enumerate(sizes):
        streams.append((0, first, 16 * size, n % 3))
        first += 16 * size
    count = len(streams)
    any_spec = pl.BlockSpec(memory_space=pl.ANY)
    out_shape = [jax.ShapeDtypeStruct((RING, RING, RING, 2, *x.shape), x.dtype) for x in shapes]
    scratch = [pltpu.SemaphoreType.DMA((12 * count,)), pltpu.SemaphoreType.DMA((12 * count,)),
               pltpu.SemaphoreType.DMA((13 * count,)), pltpu.SemaphoreType.DMA((13 * count,)),
               pltpu.SemaphoreType.DMA((count,))]
    if slots:
        blocks = (RING, RING, RING, 2, PAY, LN)
        out_shape += [jax.ShapeDtypeStruct(blocks, F32), jax.ShapeDtypeStruct((G, PAY, LN), F32)]
        scratch += [pltpu.VMEM(x.shape, x.dtype) for x in slots]
        scratch += [pltpu.VMEM((G, PAY, LN), F32), pltpu.VMEM((4, *blocks), F32),
                    pltpu.VMEM((3, 3, 2, RING, RING, 2, 8, LN), F32),
                    pltpu.SemaphoreType.DMA((55,)), pltpu.SemaphoreType.DMA((55,)), pltpu.SemaphoreType.DMA((7,)),
                    pltpu.VMEM(table.shape, table.dtype), pltpu.VMEM(gram.shape, gram.dtype),
                    pltpu.VMEM(sources[0].shape, F32)]
    else:
        scratch += [pltpu.VMEM(table.shape, table.dtype), pltpu.VMEM(gram.shape, gram.dtype), pltpu.SemaphoreType.DMA((2,))]
    tables, grams, *payload = pl.pallas_call(
        functools.partial(gather_kernel, tuple(streams), bool(slots)),
        in_specs=[any_spec] * (len(sources) + len(slots)),
        out_specs=[any_spec] * len(out_shape),
        out_shape=out_shape,
        scratch_shapes=scratch,
        compiler_params=pltpu.CompilerParams(collective_id=collective_id, has_side_effects=True),
        name='gather_all',
    )(*sources, *slots)
    return tables.reshape(G, -1, F, LN), grams.reshape(-1, LN), *payload


def half_kernel(slots, blocks, pair, lanes_of, body, emit, tab_hbm, pay_hbm, gram_hbm, x0_hbm, *refs):
    if emit:
        out_ref, tab_ref, gout_ref = refs[:3]
        refs = refs[3:]
    else:
        out_ref = refs[0]
        refs = refs[1:]
    tab, pay, ids, yu_a, yu_b, wu_a, wu_b, a_scr, at_scr, p_scr, s_scr, gpad_ref, gram_ref, x0_ref, sems = refs
    per = LN // slots
    chunks = G // per
    groups = LN // per
    steps = blocks * groups // pair
    turns = groups // pair
    heads = tab.shape[1]

    pay_copy = pltpu.make_async_copy(pay_hbm, pay, sems.at[8])
    pay_copy.start()

    def tab_copy(i):
        return pltpu.make_async_copy(tab_hbm.at[pl.ds(16 * i, 16)], tab.at[pl.ds(16 * i, 16)], sems.at[i])

    for i in range(8):
        tab_copy(i).start()
    side_copies = [pltpu.make_async_copy(gram_hbm, gram_ref, sems.at[9]), pltpu.make_async_copy(x0_hbm, x0_ref, sems.at[10])]
    for copy in side_copies:
        copy.start()
    ids[...] = iota((2 * LN, LN), 0, I16)
    pay_copy.wait()

    lane16 = iota((16, LN), 1, I16)
    lane = iota((8, LN), 1)
    row = iota((8, LN), 0)

    def sum_grams():
        for copy in side_copies:
            copy.wait()

        def add_gram(d, acc):
            return acc + gram_ref[pl.ds(pl.multiple_of(d * (F // 2), F // 2), F // 2), :]

        gram = lax.fori_loop(0, G, add_gram, jnp.zeros((F // 2, LN), F32), unroll=8)
        gpad = jnp.concatenate([unfold(gram), jnp.zeros((16, F), F32)], axis=0)
        gpad = jnp.concatenate([gpad, jnp.zeros((FX, 16), F32)], axis=1)
        rr, cc = iota((FX, FX), 0), iota((FX, FX), 1)
        gpad_ref[...] = gpad + jnp.where((rr == cc) & (rr < F), REG_LAMBDA, 0.0)

    def pay_row(t):
        if slots == 8:
            return t, 32 + t % 16, 12 * (t // 16)
        return (t % 2) * 16 + t // 2, 32 + t // 2, 12 * (t % 2)

    def spread_weights(t, wu, q):
        wrow = pay_row(t)[0]
        for c in range(chunks):
            tiles = []
            for v in range(per // 8):
                start = (per * c + 8 * v) * PAY + wrow
                tiles.append(pay[pl.ds(start, 8, stride=PAY), :])
            for bit in (1, 2, 4):
                hit = (lane & bit) != 0
                up = (row & bit) != 0
                for v in range(len(tiles)):
                    x = tiles[v]
                    if bit == 4:
                        other = pltpu.roll(x, 4, 0)
                    else:
                        other = jnp.where(up, pltpu.roll(x, bit, 0), pltpu.roll(x, 8 - bit, 0))
                    tiles[v] = jnp.where(hit, other, x)
            bit = 8
            while bit < per:
                hit = (lane & bit) != 0
                tiles = [jnp.where(hit, tiles[v ^ (bit // 8)], tiles[v]) for v in range(len(tiles))]
                bit *= 2
            for v in range(len(tiles)):
                wu[c, pl.ds(per * q + 8 * v, 8), :] = tiles[v]

    def exchange(xs, low_bit):
        bit, n = 1, len(xs)
        while bit < n:
            hit = (lane16 & I16(bit * low_bit)) != I16(0)
            xs = [jnp.where(hit, xs[a ^ bit], xs[a]) for a in range(n)]
            bit *= 2
        return xs

    ones = jnp.ones((16, LN * chunks), BF16)

    def form(y_parts, wu, u, at):
        vs = []
        for c in range(chunks):
            w = wu[c, pl.ds(u, 1), :]
            vs.append((y_parts[c].astype(F32) * w).astype(BF16))
        y = jnp.concatenate([jnp.concatenate(y_parts, axis=1), ones], axis=0)
        v = jnp.concatenate([jnp.concatenate(vs, axis=1), ones], axis=0)
        a_scr[pl.ds(at * PITCH, PITCH), pl.ds(0, FX)] = (dot_nt(y, v) + gpad_ref[...])[:PITCH]

    def form_rows(t, i, yu, wu):
        first = (t - 1) // turns % 2 * LN + (t - 1) % turns * (per * pair)
        rows = [per * (i // 4) + i % 4 + 4 * m for m in range(per // 4)]
        parts = []
        for c in range(chunks):
            by_k = [exchange([yu[u, c, pl.ds(16 * k, 16), :] for u in rows], 4) for k in range(4)]
            parts.append([jnp.concatenate([x[m] for x in by_k], axis=0) for m in range(len(rows))])
        for m, u in enumerate(rows):
            form([parts[c][m] for c in range(chunks)], wu, u, first + u)

    def codes(t, d, q):
        _, crow, shift = pay_row(pair * t + q)
        packed = pay[pl.ds(d * PAY + crow, 1), :].astype(I32)
        return (packed >> shift) & (PACK - 1)

    def by_lanes(t, d, q):
        code = jnp.broadcast_to(codes(t, d, q), (F, LN)).astype(I16)
        low = code & I16(LN - 1)
        head = code >> I16(7)
        acc = jnp.zeros((F, LN), BF16)
        for h in range(heads):
            acc = jnp.where(head == I16(h), take(tab[d, h], low, 1), acc)
        return acc

    def by_matmul(t, d):
        hots, halves = [], []
        for q in range(2):
            code = codes(t, d, q)
            low = (jnp.broadcast_to(code, (2 * LN, LN)) & (2 * LN - 1)).astype(I16)
            hots.append(jnp.where(low == ids[...], jnp.ones((2 * LN, LN), BF16), jnp.zeros((2 * LN, LN), BF16)))
            halves.append(jnp.broadcast_to(code, (F, LN)) >> 8)
        table = jnp.concatenate([jnp.concatenate([tab[d, 2 * h], tab[d, 2 * h + 1]], axis=1)
                                 for h in range(heads // 2)], axis=0)
        found = jnp.dot(table, jnp.concatenate(hots, axis=1), preferred_element_type=F32)
        out = []
        for q in range(2):
            acc = jnp.zeros((F, LN), F32)
            for h in range(heads // 2):
                acc = jnp.where(halves[q] == h, found[h * F:(h + 1) * F, q * LN:(q + 1) * LN], acc)
            out.append(acc.astype(BF16))
        return out

    def lookup(t, i, yu):
        for quad in range(4):
            found = []
            for dd in range(4):
                n = 4 * quad + dd
                d = 16 * i + n
                if (n + 1) * lanes_of // 16 > n * lanes_of // 16 if slots == 8 else n < lanes_of:
                    found.append([by_lanes(t, d, q) for q in range(pair)])
                else:
                    found.append(by_matmul(t, d))
            for q in range(pair):
                for k in range(4):
                    rows = slice(16 * k, 16 * k + 16)
                    xs = exchange([x[q][rows] for x in found], 1)
                    for a in range(4):
                        if slots == 8:
                            yu[16 * q + 4 * quad + a, i, rows, :] = xs[a]
                        else:
                            yu[64 * q + (i % 4) * 16 + 4 * quad + a, i // 4, rows, :] = xs[a]

    def flip(block, b):
        m = a_scr[pl.ds(block % 2 * (LN * PITCH) + b, LN, stride=PITCH), :].T
        at_scr[b] = m[:F]
        s_scr[pl.ds(b, 1), :] = m[F:F + 1]

    def flip_all(block):
        def four(b4, _):
            for e in range(4):
                flip(block, 4 * b4 + e)
            return 0

        lax.fori_loop(0, F // 4, four, 0)

    def solve(block):
        rhs = a_scr[pl.ds(block % 2 * (LN * PITCH) + F, LN, stride=PITCH), :].T[:F] + s_scr[...]
        x = x0_ref[:, pl.ds(pl.multiple_of(block * LN, LN), LN)]

        def apply_mat(vec):
            p_scr[...] = vec

            def add(b, acc):
                return acc + at_scr[b] * p_scr[pl.ds(b, 1), :]

            return lax.fori_loop(0, F, add, jnp.zeros((F, LN), F32), unroll=16)

        res = rhs - apply_mat(x)
        direction = res
        res_sq = jnp.sum(res * res, axis=0, keepdims=True)
        for step in range(CG_STEPS):
            q = apply_mat(direction)
            length = res_sq / jnp.sum(direction * q, axis=0, keepdims=True)
            x = x + length * direction
            if step + 1 < CG_STEPS:
                res = res - length * q
                new_sq = jnp.sum(res * res, axis=0, keepdims=True)
                direction = res + (new_sq / res_sq) * direction
                res_sq = new_sq
        out_ref[:, pl.ds(pl.multiple_of(block * LN, LN), LN)] = x
        if emit:
            xb = x.astype(BF16)
            tab_ref[block] = xb
            gout_ref[...] += fold(dot_nt(xb, xb))

    if emit:
        gout_ref[...] = jnp.zeros((F // 2, LN), F32)

    def weights(t, wu):
        for q in range(pair):
            spread_weights(pair * t + q, wu, q)

    def first_pass():
        weights(0, wu_a)

        def inner(i, _):
            tab_copy(i).wait()
            lookup(0, i, yu_a)
            return 0

        lax.fori_loop(0, 8, inner, 0)

    def step_pass(t, ahead, count, size, yu, wu, yu_last, wu_last):
        before = jnp.maximum((t - 1) // turns - 1, 0)
        if ahead:
            weights(jnp.minimum(t, steps - 1), wu)

        def inner(i2, _):
            flips = F // (8 * turns)
            for i in range(size):
                i = size * i2 + i
                for e in range(flips):
                    flip(before, ((t - 1) % turns * 8 + i) * flips + e)
                jobs = [functools.partial(form_rows, t, i, yu_last, wu_last)]
                if ahead:
                    jobs.insert(0 if body > 1 else 1, functools.partial(lookup, t, i, yu))
                for job in jobs:
                    job()
            return 0

        lax.fori_loop(0, count, inner, 0)

        def finish_block():
            @pl.when((t >= turns + 1) & (t % turns == 0))
            def _():
                solve(t // turns - 2)

        if ahead:
            pl.when(t < steps)(finish_block)
        else:
            finish_block()

    def two_steps(j, _):
        step_pass(2 * j + 1, True, 8 // body, body, yu_b, wu_b, yu_a, wu_a)
        step_pass(2 * j + 2, True, jnp.where(2 * j + 2 < steps, 8 // body, 0), body, yu_a, wu_a, yu_b, wu_b)
        return 0

    first_pass()
    sum_grams()
    lax.fori_loop(0, steps // 2, two_steps, 0)
    step_pass(steps, False, 8, 1, None, None, yu_b, wu_b)
    flip_all(blocks - 1)
    solve(blocks - 1)


def half_step(slots, emit, pair, lanes_of, body, tables, payload, gram, x0_t):
    n = x0_t.shape[1]
    heads = tables.shape[1]
    per = LN // slots
    chunks = G // per
    out_shape = [jax.ShapeDtypeStruct((F, n), F32)]
    if emit:
        out_shape += [jax.ShapeDtypeStruct((n // LN, F, LN), BF16), jax.ShapeDtypeStruct((F // 2, LN), F32)]
    vmem = pl.BlockSpec(memory_space=pltpu.VMEM)
    return pl.pallas_call(
        functools.partial(half_kernel, slots, n // LN, pair, lanes_of, body, emit),
        in_specs=[pl.BlockSpec(memory_space=pl.ANY)] * 4,
        out_specs=[vmem] * len(out_shape),
        out_shape=out_shape,
        scratch_shapes=[
            pltpu.VMEM((G, heads, F, LN), BF16),
            pltpu.VMEM((G * PAY, LN), F32),
            pltpu.VMEM((2 * LN, LN), I16),
            pltpu.VMEM((pair * per, chunks, F, LN), BF16),
            pltpu.VMEM((pair * per, chunks, F, LN), BF16),
            pltpu.VMEM((chunks, pair * per, LN), F32),
            pltpu.VMEM((chunks, pair * per, LN), F32),
            pltpu.VMEM((2 * LN * PITCH, LN), F32),
            pltpu.VMEM((F, F, LN), F32),
            pltpu.VMEM((F, LN), F32),
            pltpu.VMEM((F, LN), F32),
            pltpu.VMEM((FX, FX), F32),
            pltpu.VMEM(gram.shape, F32),
            pltpu.VMEM(x0_t.shape, F32),
            pltpu.SemaphoreType.DMA((11,)),
        ],
        compiler_params=pltpu.CompilerParams(vmem_limit_bytes=62 * 1024 * 1024),
        cost_estimate=pl.CostEstimate(flops=10 ** 11, bytes_accessed=2 ** 25, transcendentals=0),
        name='half_step',
    )(tables, payload, gram, x0_t)


def solution(mesh):
    part_spec = P(('tables', 'g'), None)
    slot_spec = P(('tables', 'g'), None, None)

    def local_sweep(item_block, start_block, item_idx, item_conf, user_idx, user_conf):
        item_t = item_block.T

        def as_rows(x):
            return x[0].reshape(-1, LN, 2).transpose(0, 2, 1).reshape(-1, LN)

        gram_shape = jax.ShapeDtypeStruct((F // 2, LN), F32)
        tables, gram_items, payload, late = gather_all(
            (item_t,), (jax.ShapeDtypeStruct((item_t.size // LN, LN), BF16), gram_shape), 0,
            (item_idx[0].T, item_conf[0].T, as_rows(user_idx), as_rows(user_conf)))
        late = lax.all_to_all(late, 'g', 0, 0, tiled=True)
        user_t, user_table, gram_part = half_step(8, True, 2, 6, 2, tables, payload.reshape(G * PAY, LN),
                                                  gram_items, start_block.T)
        user_table = user_table.reshape(-1, LN)
        user_tables, gram_users = gather_all((user_table, gram_part), (user_table, gram_part), 1)
        item_new = half_step(2, False, 2, 6, 1, user_tables, late.reshape(G * PAY, LN), gram_users, item_t)[0]
        return user_t.T, item_new.T

    return jax.shard_map(local_sweep, mesh=mesh,
                         in_specs=(part_spec, part_spec, slot_spec, slot_spec, slot_spec, slot_spec),
                         out_specs=(part_spec, part_spec), check_vma=False)
```
